128 devices in a mesh: row: 4 (over y), col: 32 (over z, x, core).
Axes of the slice: x: 4, y: 4, z: 4, core: 2. Of those that a mesh axis runs over, the one named last changes fastest.
Arguments:
- node_features: bfloat16 [8192, 128, 512], P(('row', 'col')), may hold values from -6 to 6
- node_counts: int32 [8192], P(('row', 'col')), may hold values from 16 to 128, as said below
- edge_list: int32 [8192, 2, 256], P(('row', 'col')), may hold values from 0 to 128, as said below
- readout_ids: int32 [8192], P(('row', 'col')), may hold values from 0 to 1023
- live_graphs: int32 [128], P(('row', 'col')), may hold values from 1 to 64, as said below
- self_weight: float32 [1], replicated, may hold values from 0.5 to 1.5
- w_first: bfloat16 [512, 512], replicated, may hold values from -0.25 to 0.25
- b_first: float32 [512], replicated, may hold values from -3 to 3
- w_second: bfloat16 [512, 512], replicated, may hold values from -0.25 to 0.25
- b_second: float32 [512], replicated, may hold values from -3 to 3
- w_third: bfloat16 [512, 512], replicated, may hold values from -0.25 to 0.25
- b_third: float32 [512], replicated, may hold values from -3 to 3
Outputs:
- node_out: bfloat16 [4096, 128, 512], P(('row', 'col'))
- readout: float32 [1024, 512], P(('row', 'col'))
The draws below stay inside these ranges and needn't reach their ends.
Inputs may be any that keep to these rules, and one draw needn't show every extreme that they name: `live_graphs`: the entries sum to 4096, and at least one equals 64. `node_counts`: node slots 0 to count - 1 of a graph are live; the rest of its block is padding. `edge_list`: each edge slot holds two node indices below its graph's node count, or 128 in both rows for an unused slot.
All inputs are finite; a program needn't handle non-finite values.
Results may differ from the reference program's by a relative error of at most 0.0058.
Values may be sent and summed in bfloat16 or wider, within the bound.
No kernel may reach another device: no remote copies, remote signals or barrier semaphores. Data moves between devices by JAX's collectives and lax.ppermute only.
A program may use at most 128 MiB of HBM per device.

```python
import jax
import jax.numpy as jnp
from jax import lax

H = 512
BLOCK = 128
G_DEV = 32
MIN_NODES = 16
CAP_IN = 64
GRAPHS = 4096
GRAPHS_IN = 8192
READOUTS = 1024
DEVICES = 128


def graph_shapes(key):
    folded = jax.random.fold_in(key, 11)
    counts = jax.random.randint(jax.random.fold_in(folded, 1), (GRAPHS_IN,), MIN_NODES, BLOCK + 1, dtype=jnp.int32)
    pair_total = jax.random.randint(jax.random.fold_in(folded, 2), (GRAPHS_IN,), counts // 2, counts + 1, dtype=jnp.int32)
    ends_first = jax.random.randint(jax.random.fold_in(folded, 3), (GRAPHS_IN, BLOCK), 0, counts[:, None], dtype=jnp.int32)
    ends_second = jax.random.randint(jax.random.fold_in(folded, 4), (GRAPHS_IN, BLOCK), 0, counts[:, None], dtype=jnp.int32)
    pair_index = jnp.arange(BLOCK, dtype=jnp.int32)[None, :]
    pair_used = jnp.concatenate([pair_index < pair_total[:, None], pair_index < pair_total[:, None]], axis=1)
    sources = jnp.where(pair_used, jnp.concatenate([ends_first, ends_second], axis=1), BLOCK)
    targets = jnp.where(pair_used, jnp.concatenate([ends_second, ends_first], axis=1), BLOCK)
    return (counts, jnp.stack([sources, targets], axis=1).astype(jnp.int32))


def draw_node_counts(key, part):
    return graph_shapes(key)[0]


def draw_edge_list(key, part):
    return graph_shapes(key)[1]


def draw_live_graphs(key, part):
    halves = DEVICES // 2
    shuffled = jax.random.permutation(jax.random.fold_in(key, 23), DEVICES)
    moves = jax.random.randint(jax.random.fold_in(key, 29), (halves,), 0, G_DEV, dtype=jnp.int32)
    moves = moves.at[0].set(G_DEV - 1)
    higher = G_DEV + moves
    lower = G_DEV - moves
    higher = higher.at[0].add(1)
    higher = higher.at[1].add(-1)
    counts = jnp.zeros((DEVICES,), jnp.int32)
    counts = counts.at[shuffled[0::2]].set(higher)
    counts = counts.at[shuffled[1::2]].set(lower)
    return counts.astype(jnp.int32)


def set_ends(values, own_key, smallest, largest):
    extent = values.shape
    place = [jax.random.randint(jax.random.fold_in(own_key, axis), (), 0, extent[axis]) for axis in range(len(extent))]
    values = values.at[tuple(place)].set(smallest)
    longest = extent.index(max(extent))
    place[longest] = (place[longest] + 1) % extent[longest]
    return values.at[tuple(place)].set(largest)


def levels(key, shape, pieces, least, high):
    gain, own = 1.0, jax.random.fold_in(key, 6)
    for position, blocks in pieces:
        steps = jnp.exp(jax.random.uniform(jax.random.fold_in(own, position), (blocks,), jnp.float32, least / len(pieces), high / len(pieces)))
        gain = gain * jnp.repeat(steps, shape[position] // blocks).reshape([-1 if axis == position else 1 for axis in range(len(shape))])
    return gain


def normal_values(key, dims, spread, reach, pieces=(), kind=jnp.bfloat16):
    values = jax.random.normal(key, dims, jnp.float32) * spread
    if len(pieces) > 0:
        values = levels(key, dims, pieces, -0.22, 0.18) * values
    return jnp.clip(values, min=-reach, max=reach).astype(kind)


def setup_inputs(seed: int = 0) -> dict:
    splits = jax.random.split(jax.random.key(seed), 13)
    node_features = normal_values(splits[0], (GRAPHS_IN, BLOCK, H), 1.0, 6.0, ((0, 128),))
    node_counts = draw_node_counts(jax.random.fold_in(splits[12], 71), 0)
    edge_list = draw_edge_list(jax.random.fold_in(splits[12], 71), 0)
    readout_ids = set_ends(jax.random.randint(splits[3], (GRAPHS_IN,), 0, READOUTS), jax.random.fold_in(splits[3], 1), 0, READOUTS - 1).astype(jnp.int32)
    live_graphs = draw_live_graphs(jax.random.fold_in(splits[12], 71), 0)
    self_weight = jnp.clip(jax.random.uniform(splits[5], (1,), jnp.float32, 0.5, 1.5), 0.5, 1.5)
    w_first = normal_values(splits[6], (H, H), H ** -0.5, 0.25)
    b_first = normal_values(splits[7], (H,), 0.5, 3.0, (), jnp.float32)
    w_second = normal_values(splits[8], (H, H), H ** -0.5, 0.25)
    b_second = normal_values(splits[9], (H,), 0.5, 3.0, (), jnp.float32)
    w_third = normal_values(splits[10], (H, H), H ** -0.5, 0.25)
    b_third = normal_values(splits[11], (H,), 0.5, 3.0, (), jnp.float32)
    return {"node_features": node_features, "node_counts": node_counts, "edge_list": edge_list, "readout_ids": readout_ids, "live_graphs": live_graphs, "self_weight": self_weight, "w_first": w_first, "b_first": b_first, "w_second": w_second, "b_second": b_second, "w_third": w_third, "b_third": b_third}


def blend_nodes(features, edge_slots, self_weight):
    node_index = jnp.arange(BLOCK, dtype=jnp.int32)
    sources = (edge_slots[:, 0, :, None] == node_index[None, None, :]).astype(jnp.float32)
    targets = (edge_slots[:, 1, :, None] == node_index[None, None, :]).astype(jnp.float32)
    adjacency = jnp.einsum("gek,gel->gkl", targets, sources)
    neighbour = jnp.einsum("gkl,glh->gkh", adjacency, features.astype(jnp.float32))
    return (self_weight[0] * features.astype(jnp.float32) + neighbour).astype(jnp.bfloat16)


def perceptron(blended, weights):
    w_first, b_first, w_second, b_second, w_third, b_third = weights
    flat_rows = blended.reshape(-1, blended.shape[-1])
    hidden_one = jax.nn.relu(jnp.dot(flat_rows, w_first, preferred_element_type=jnp.float32) + b_first).astype(jnp.bfloat16)
    hidden_two = jax.nn.relu(jnp.dot(hidden_one, w_second, preferred_element_type=jnp.float32) + b_second).astype(jnp.bfloat16)
    result = jnp.dot(hidden_two, w_third, preferred_element_type=jnp.float32) + b_third
    return result.reshape(blended.shape)


def source_rows(live_graphs):
    inclusive = jnp.cumsum(live_graphs).astype(jnp.int32)
    offsets = (inclusive - live_graphs).astype(jnp.int32)
    order_index = jnp.arange(GRAPHS, dtype=jnp.int32)
    number = (order_index % G_DEV) * DEVICES + order_index // G_DEV
    source = jnp.sum((inclusive[None, :] <= number[:, None]).astype(jnp.int32), axis=1).astype(jnp.int32)
    return (source * CAP_IN + number - offsets[source]).astype(jnp.int32)


def reference(node_features, node_counts, edge_list, readout_ids, live_graphs, self_weight, w_first, b_first, w_second, b_second, w_third, b_third):
    weights = (w_first, b_first, w_second, b_second, w_third, b_third)
    chosen = source_rows(live_graphs).reshape(DEVICES, G_DEV)

    def one_group(indices):
        features = node_features[indices]
        counts_here = node_counts[indices]
        blended = blend_nodes(features, edge_list[indices], self_weight)
        live_nodes = jnp.arange(BLOCK, dtype=jnp.int32)[None, :] < counts_here[:, None]
        outputs = jnp.where(live_nodes[:, :, None], perceptron(blended, weights), 0.0).astype(jnp.bfloat16)
        pooled = jnp.sum(outputs.astype(jnp.float32), axis=1) / counts_here[:, None].astype(jnp.float32)
        return outputs, pooled

    node_out, pooled = lax.map(one_group, chosen)
    node_out = node_out.reshape(GRAPHS, BLOCK, H)
    pooled = pooled.reshape(GRAPHS, H)
    graph_ids = readout_ids[chosen.reshape(-1)]
    id_keys = jnp.arange(READOUTS, dtype=jnp.int32)
    members = (id_keys[:, None] == graph_ids[None, :]).astype(jnp.float32)
    readout = jnp.dot(members, pooled, precision=lax.Precision.HIGHEST, preferred_element_type=jnp.float32)
    return node_out, readout
```

```python
import functools

import jax
import jax.numpy as jnp
from jax import lax
from jax.experimental import pallas as pl
from jax.experimental.pallas import tpu as pltpu
from jax.sharding import Mesh
from jax.sharding import PartitionSpec as P

G_DEV = 32
READ_DEV = 8
ROW_COL = ("row", "col_0", "col_1", "col_2")
CHIP = ("row", "col_0", "col_1")
SWAP = [(0, 1), (1, 0)]
PACK = 4
POOL = 8
MLP = 4


def masked_sum(keep, values, axis):
    return jnp.sum(jnp.where(keep, values, 0), axis=axis)


def blend_kernel(own_idx, par_idx, from_par, scale, *refs):
    owns, pars = refs[:PACK], refs[PACK : 2 * PACK]
    own_edges, par_edges, out = refs[2 * PACK :]
    step = pl.program_id(0)
    nodes = owns[0].shape[1]
    slots = own_edges.shape[-1]
    node_index = lax.broadcasted_iota(jnp.int32, (nodes, slots), 0)
    for lane in range(PACK):
        slot = step * PACK + lane
        pick = from_par[slot] == 1
        features = jnp.where(pick, pars[lane][0], owns[lane][0])
        edges = jnp.where(pick, par_edges[par_idx[slot]], own_edges[own_idx[slot]])
        sources = (node_index == edges[0:1, :]).astype(jnp.bfloat16)
        targets = (node_index == edges[1:2, :]).astype(jnp.bfloat16)
        adjacency = lax.dot_general(
            targets, sources, (((1,), (1,)), ((), ())), preferred_element_type=jnp.float32
        ).astype(jnp.bfloat16)
        neighbour = jnp.dot(adjacency, features, preferred_element_type=jnp.float32)
        out[lane] = (scale[0] * features.astype(jnp.float32) + neighbour).astype(jnp.bfloat16)


def blended_slots(own, par, own_edges, par_edges, own_idx, par_idx, from_par, scale):
    slots, nodes, hidden = own.shape
    count = own_idx.shape[0]

    def picked(table, lane):
        return pl.BlockSpec(
            (1, nodes, hidden), lambda i, *tables: (tables[table][i * PACK + lane], 0, 0)
        )

    whole = pl.BlockSpec(own_edges.shape, lambda i, *tables: (0, 0, 0))
    return pl.pallas_call(
        blend_kernel,
        out_shape=jax.ShapeDtypeStruct((count, nodes, hidden), jnp.bfloat16),
        grid_spec=pltpu.PrefetchScalarGridSpec(
            num_scalar_prefetch=4,
            grid=(count // PACK,),
            in_specs=[picked(0, lane) for lane in range(PACK)]
            + [picked(1, lane) for lane in range(PACK)]
            + [whole, whole],
            out_specs=pl.BlockSpec((PACK, nodes, hidden), lambda i, *tables: (i, 0, 0)),
        ),
        compiler_params=pltpu.CompilerParams(dimension_semantics=("arbitrary",)),
        cost_estimate=pl.CostEstimate(
            flops=2 * count * nodes * nodes * (own_edges.shape[-1] + hidden),
            bytes_accessed=4 * count * nodes * hidden,
            transcendentals=0,
        ),
        name="blend",
    )(own_idx, par_idx, from_par, scale, *[own] * PACK, *[par] * PACK, own_edges, par_edges)


def perceptron(rows, weights):
    w_first, b_first, w_second, b_second, w_third, b_third = weights
    for w, b in ((w_first, b_first), (w_second, b_second)):
        total = jnp.dot(rows, w[...], preferred_element_type=jnp.float32) + b[...]
        rows = jnp.maximum(total, 0.0).astype(jnp.bfloat16)
    return jnp.dot(rows, w_third[...], preferred_element_type=jnp.float32) + b_third[...]


def weight_specs(weights):
    return [pl.BlockSpec(w.shape, lambda i, *tables: (0, 0)) for w in weights]


def mlp_cost(rows, hidden):
    return pl.CostEstimate(
        flops=6 * rows * hidden * hidden, bytes_accessed=4 * rows * hidden, transcendentals=0
    )


def pool_kernel(counts, rows_ref, *refs):
    weights, out = refs[:6], refs[6]
    step = pl.program_id(0)
    many, nodes, hidden = rows_ref.shape
    result = perceptron(rows_ref[...].reshape(many * nodes, hidden), weights)
    node_index = lax.broadcasted_iota(jnp.int32, (nodes, 1), 0)
    for lane in range(many):
        count = counts[step * many + lane]
        part = result[lane * nodes : (lane + 1) * nodes]
        kept = jnp.where(node_index < count, part, 0.0).astype(jnp.bfloat16).astype(jnp.float32)
        shown = jnp.maximum(count, 1).astype(jnp.float32)
        out[lane : lane + 1, :] = jnp.sum(kept, axis=0, keepdims=True) / shown


def pooled_slots(blended, counts, weights):
    count, nodes, hidden = blended.shape
    return pl.pallas_call(
        pool_kernel,
        out_shape=jax.ShapeDtypeStruct((count, hidden), jnp.float32),
        grid_spec=pltpu.PrefetchScalarGridSpec(
            num_scalar_prefetch=1,
            grid=(count // POOL,),
            in_specs=[pl.BlockSpec((POOL, nodes, hidden), lambda i, *tables: (i, 0, 0))]
            + weight_specs(weights),
            out_specs=pl.BlockSpec((POOL, hidden), lambda i, *tables: (i, 0)),
        ),
        compiler_params=pltpu.CompilerParams(dimension_semantics=("arbitrary",)),
        cost_estimate=mlp_cost(count * nodes, hidden),
        name="pool",
    )(counts, blended, *weights)


def place_kernel(chips, counts, *refs):
    blocks, weights, out = refs[:MLP], refs[MLP : MLP + 6], refs[MLP + 6]
    step = pl.program_id(0)
    nodes = out.shape[1]
    rows = jnp.concatenate([block[0] for block in blocks], axis=0)
    result = perceptron(rows, weights)
    node_index = lax.broadcasted_iota(jnp.int32, (nodes, 1), 0)
    for lane in range(MLP):
        part = result[lane * nodes : (lane + 1) * nodes]
        live = node_index < counts[step * MLP + lane]
        out[lane] = jnp.where(live, part, 0.0).astype(jnp.bfloat16)


def placed_nodes(arrived, chips, counts, weights):
    _, nodes, hidden = arrived.shape

    def picked(lane):
        return pl.BlockSpec(
            (1, nodes, hidden), lambda i, *tables: (tables[0][i * MLP + lane], 0, 0)
        )

    return pl.pallas_call(
        place_kernel,
        out_shape=jax.ShapeDtypeStruct((G_DEV, nodes, hidden), jnp.bfloat16),
        grid_spec=pltpu.PrefetchScalarGridSpec(
            num_scalar_prefetch=2,
            grid=(G_DEV // MLP,),
            in_specs=[picked(lane) for lane in range(MLP)] + weight_specs(weights),
            out_specs=pl.BlockSpec((MLP, nodes, hidden), lambda i, *tables: (i, 0, 0)),
        ),
        compiler_params=pltpu.CompilerParams(dimension_semantics=("arbitrary",)),
        cost_estimate=mlp_cost(G_DEV * nodes, hidden),
        name="place",
    )(chips, counts, *[arrived] * MLP, *weights)


def sum_over_axis(blocks, axis):
    size = lax.axis_size(axis)
    me = lax.axis_index(axis)
    rounded = blocks.astype(jnp.bfloat16)
    total = lax.dynamic_index_in_dim(blocks, me, 0, keepdims=False).astype(jnp.float32)
    for shift in range(1, size):
        part = lax.dynamic_index_in_dim(rounded, (me + shift) % size, 0, keepdims=False)
        ring = [(i, (i + shift) % size) for i in range(size)]
        total = total + lax.ppermute(part, axis, ring).astype(jnp.float32)
    return total


def body(
    node_features,
    node_counts,
    edge_list,
    readout_ids,
    live_graphs,
    self_weight,
    w_first,
    b_first,
    w_second,
    b_second,
    w_third,
    b_third,
):
    weights = (
        w_first,
        b_first[None, :],
        w_second,
        b_second[None, :],
        w_third,
        b_third[None, :],
    )
    devices = lax.axis_size(ROW_COL)
    capacity, nodes, hidden = node_features.shape
    me = lax.axis_index(ROW_COL)
    core = lax.axis_index("col_2")
    chip = me // 2

    par_features = lax.ppermute(node_features, "col_2", SWAP)
    par_edges = lax.ppermute(edge_list, "col_2", SWAP)
    info = jnp.concatenate([live_graphs, node_counts, readout_ids])
    table = lax.all_to_all(
        jnp.broadcast_to(info[None], (devices, info.shape[0])), ROW_COL, 0, 0, tiled=True
    )
    live = table[:, 0]
    all_counts = table[:, 1 : 1 + capacity]

    device = lax.broadcasted_iota(jnp.int32, (devices,), 0)
    chip_offset = masked_sum(device < 2 * chip, live, 0)
    live_a = masked_sum(device == 2 * chip, live, 0)
    live_b = masked_sum(device == 2 * chip + 1, live, 0)
    slot = lax.broadcasted_iota(jnp.int32, (devices // 2,), 0)
    number = (2 * slot + core - chip_offset) % devices
    idx_a = jnp.clip(number, 0, live_a - 1)
    idx_b = jnp.clip(number - live_a, 0, live_b - 1)
    from_b = number >= live_a
    filled = number < live_a + live_b
    own_idx = jnp.where(core == 0, idx_a, idx_b)
    par_idx = jnp.where(core == 0, idx_b, idx_a)
    from_par = jnp.where(core == 0, from_b, ~from_b).astype(jnp.int32)

    blended = blended_slots(
        node_features, par_features, edge_list, par_edges, own_idx, par_idx, from_par, self_weight
    )
    arrived = lax.all_to_all(blended, CHIP, split_axis=0, concat_axis=0, tiled=True)

    pair = lax.dynamic_slice_in_dim(table, 2 * chip, 2, 0)
    picked = jnp.where(from_b, capacity + idx_b, idx_a)
    spot = lax.broadcasted_iota(jnp.int32, (devices // 2, 2 * capacity), 1) == picked[:, None]
    slot_counts = masked_sum(spot, pair[:, 1 : 1 + capacity].reshape(1, -1), 1)
    slot_ids = masked_sum(spot, pair[:, 1 + capacity :].reshape(1, -1), 1)
    slot_ids = jnp.where(filled, slot_ids, -1)
    pooled = pooled_slots(blended, slot_counts, weights)
    groups = READ_DEV * devices
    id_keys = lax.broadcasted_iota(jnp.int32, (groups, slot_ids.shape[0]), 0)
    members = (id_keys == slot_ids[None, :]).astype(jnp.float32)
    terms = jnp.dot(
        members, pooled, precision=lax.Precision.HIGHEST, preferred_element_type=jnp.float32
    )
    terms = terms.astype(jnp.bfloat16).reshape(devices // 2, 2, READ_DEV, hidden).swapaxes(0, 1)
    sums = sum_over_axis(terms, "col_2")
    sums = sums.reshape(devices // 8, 4, READ_DEV, hidden).swapaxes(0, 1)
    sums = sum_over_axis(sums, "col_1")
    sums = sums.reshape(devices // 32, 4, READ_DEV, hidden).swapaxes(0, 1)
    sums = sum_over_axis(sums, "col_0")
    readout = sum_over_axis(sums, "row")

    order = lax.broadcasted_iota(jnp.int32, (G_DEV, 1), 0) * devices + me
    upto = masked_sum(device[None, :] <= device[:, None], live[None, :], 1)
    passed = upto[None, :] <= order
    source = jnp.sum(passed.astype(jnp.int32), axis=1)
    start = jnp.max(jnp.where(passed, upto[None, :], 0), axis=1)
    source_idx = order[:, 0] - start
    hit = (device[None, :, None] == source[:, None, None]) & (
        lax.broadcasted_iota(jnp.int32, (1, 1, capacity), 2) == source_idx[:, None, None]
    )
    counts = jnp.sum(jnp.where(hit, all_counts[None], 0), axis=(1, 2))
    node_out = placed_nodes(arrived, source // 2, counts, weights)
    return (node_out, readout)


def solution(mesh):
    split = Mesh(
        mesh.devices.reshape(mesh.shape["row"], 4, 4, 2), ("row", "col_0", "col_1", "col_2")
    )
    return jax.shard_map(
        body,
        mesh=split,
        in_specs=(
            P(ROW_COL, None, None),
            P(ROW_COL),
            P(ROW_COL, None, None),
            P(ROW_COL),
            P(ROW_COL),
            P(),
            P(),
            P(),
            P(),
            P(),
            P(),
            P(),
        ),
        out_specs=(P(ROW_COL, None, None), P(ROW_COL, None)),
        check_vma=False,
    )
```

```python
import jax
import jax.numpy as jnp
from jax import lax
from jax.experimental import pallas as pl
from jax.experimental.pallas import tpu as pltpu
from jax.sharding import Mesh
from jax.sharding import PartitionSpec as P

G_DEV = 32
READ_DEV = 8
ROW_COL = ("row", "col_0", "col_1", "col_2")
CHIP = ("row", "col_0", "col_1")
SWAP = [(0, 1), (1, 0)]
PACK_BITS = 3
PACK = 1 << PACK_BITS
POOL = 8
MLP_BITS = 2
MLP = 1 << MLP_BITS
VMEM_BYTES = 58 * 1024 * 1024


def masked_sum(keep, values, axis):
    return jnp.sum(jnp.where(keep, values, 0), axis=axis)


def blend_kernel(
    where, scale, own, par, own_edges, par_edges, out, taken, made, taken_sem, made_sem
):
    core, offset, live_a, live_b = where[0], where[1], where[2], where[3]
    count, nodes, _ = taken.shape
    wrap = 2 * count - 1
    node_index = lax.broadcasted_iota(jnp.int32, (nodes, own_edges.shape[-1]), 0)

    def source_of(slot):
        number = (2 * slot + core - offset) & wrap
        filled = number < live_a + live_b
        from_b = number >= live_a
        index = jnp.where(filled, jnp.where(from_b, number - live_a, number), slot)
        return index, jnp.logical_xor(from_b, core == 1)

    @pl.loop(0, count)
    def _(slot):
        index, from_par = source_of(slot)
        sem = taken_sem.at[slot >> PACK_BITS]

        @pl.when(from_par)
        def _():
            pltpu.make_async_copy(par.at[index], taken.at[slot], sem).start()

        @pl.when(jnp.logical_not(from_par))
        def _():
            pltpu.make_async_copy(own.at[index], taken.at[slot], sem).start()

    def put(group):
        rows = pl.ds(group * PACK, PACK)
        return pltpu.make_async_copy(made.at[rows], out.at[rows], made_sem.at[group])

    @pl.loop(0, count // PACK)
    def _(group):
        pltpu.make_async_copy(
            own.at[pl.ds(0, PACK)], taken.at[pl.ds(group * PACK, PACK)], taken_sem.at[group]
        ).wait()
        slots = [group * PACK + lane for lane in range(PACK)]
        sources, targets = [], []
        for slot in slots:
            index, from_par = source_of(slot)
            edges = jnp.where(from_par, par_edges[index], own_edges[index])
            sources.append((node_index == edges[0:1, :]).astype(jnp.bfloat16))
            targets.append((node_index == edges[1:2, :]).astype(jnp.bfloat16))
        adjacency = [
            lax.dot_general(t, s, (((1,), (1,)), ((), ())), preferred_element_type=jnp.float32)
            for t, s in zip(targets, sources)
        ]
        features = [taken[slot] for slot in slots]
        neighbours = [
            jnp.dot(a.astype(jnp.bfloat16), f, preferred_element_type=jnp.float32)
            for a, f in zip(adjacency, features)
        ]
        for slot, f, n in zip(slots, features, neighbours):
            made[slot] = (scale[0] * f.astype(jnp.float32) + n).astype(jnp.bfloat16)
        put(group).start()

    @pl.loop(0, count // PACK)
    def _(group):
        put(group).wait()


def blended_slots(own, par, own_edges, par_edges, where, scale):
    count, nodes, hidden = own.shape
    anywhere = pl.BlockSpec(memory_space=pl.ANY)
    vector = pl.BlockSpec(memory_space=pltpu.VMEM)
    scalar = pl.BlockSpec(memory_space=pltpu.SMEM)
    return pl.pallas_call(
        blend_kernel,
        out_shape=jax.ShapeDtypeStruct((count, nodes, hidden), jnp.bfloat16),
        in_specs=[scalar, scalar, anywhere, anywhere, vector, vector],
        out_specs=anywhere,
        scratch_shapes=[
            pltpu.VMEM((count, nodes, hidden), jnp.bfloat16),
            pltpu.VMEM((count, nodes, hidden), jnp.bfloat16),
            pltpu.SemaphoreType.DMA((count // PACK,)),
            pltpu.SemaphoreType.DMA((count // PACK,)),
        ],
        compiler_params=pltpu.CompilerParams(vmem_limit_bytes=VMEM_BYTES),
        cost_estimate=pl.CostEstimate(
            flops=2 * count * nodes * nodes * (own_edges.shape[-1] + hidden),
            bytes_accessed=4 * count * nodes * hidden,
            transcendentals=0,
        ),
        name="blend",
    )(where, scale, own, par, own_edges, par_edges)


def perceptron(rows, weights):
    w_first, b_first, w_second, b_second, w_third, b_third = weights
    for w, b in ((w_first, b_first), (w_second, b_second)):
        total = jnp.dot(rows, w[...], preferred_element_type=jnp.float32) + b[...]
        rows = jnp.maximum(total, 0.0).astype(jnp.bfloat16)
    return jnp.dot(rows, w_third[...], preferred_element_type=jnp.float32) + b_third[...]


def weight_specs(weights):
    return [pl.BlockSpec(w.shape, lambda i, *tables: (0, 0)) for w in weights]


def mlp_cost(rows, hidden):
    return pl.CostEstimate(
        flops=6 * rows * hidden * hidden, bytes_accessed=4 * rows * hidden, transcendentals=0
    )


def pool_kernel(counts, rows_ref, *refs):
    weights, out = refs[:6], refs[6]
    step = pl.program_id(0)
    many, nodes, hidden = rows_ref.shape
    result = perceptron(rows_ref[...].reshape(many * nodes, hidden), weights)
    node_index = lax.broadcasted_iota(jnp.int32, (nodes, 1), 0)
    for lane in range(many):
        count = counts[step * many + lane]
        part = result[lane * nodes : (lane + 1) * nodes]
        kept = jnp.where(node_index < count, part, 0.0).astype(jnp.bfloat16).astype(jnp.float32)
        shown = jnp.maximum(count, 1).astype(jnp.float32)
        out[lane : lane + 1, :] = jnp.sum(kept, axis=0, keepdims=True) / shown


def pooled_slots(blended, counts, weights):
    count, nodes, hidden = blended.shape
    return pl.pallas_call(
        pool_kernel,
        out_shape=jax.ShapeDtypeStruct((count, hidden), jnp.float32),
        grid_spec=pltpu.PrefetchScalarGridSpec(
            num_scalar_prefetch=1,
            grid=(count // POOL,),
            in_specs=[pl.BlockSpec((POOL, nodes, hidden), lambda i, *tables: (i, 0, 0))]
            + weight_specs(weights),
            out_specs=pl.BlockSpec((POOL, hidden), lambda i, *tables: (i, 0)),
        ),
        compiler_params=pltpu.CompilerParams(dimension_semantics=("arbitrary",)),
        cost_estimate=mlp_cost(count * nodes, hidden),
        name="pool",
    )(counts, blended, *weights)


def place_kernel(chips, counts, arrived, *refs):
    weights, out, taken, made, taken_sem, made_sem = refs[:6], *refs[6:]
    count, nodes, hidden = taken.shape

    @pl.loop(0, count)
    def _(slot):
        pltpu.make_async_copy(
            arrived.at[chips[slot]], taken.at[slot], taken_sem.at[slot >> MLP_BITS]
        ).start()

    def put(group):
        rows = pl.ds(group * MLP, MLP)
        return pltpu.make_async_copy(made.at[rows], out.at[rows], made_sem.at[group])

    node_index = lax.broadcasted_iota(jnp.int32, (nodes, 1), 0)

    @pl.loop(0, count // MLP)
    def _(group):
        rows = pl.ds(group * MLP, MLP)
        pltpu.make_async_copy(
            arrived.at[pl.ds(0, MLP)], taken.at[rows], taken_sem.at[group]
        ).wait()
        result = perceptron(taken[rows].reshape(MLP * nodes, hidden), weights)
        for lane in range(MLP):
            slot = group * MLP + lane
            part = result[lane * nodes : (lane + 1) * nodes]
            made[slot] = jnp.where(node_index < counts[slot], part, 0.0).astype(jnp.bfloat16)
        put(group).start()

    @pl.loop(0, count // MLP)
    def _(group):
        put(group).wait()


def placed_nodes(arrived, chips, counts, weights):
    _, nodes, hidden = arrived.shape
    anywhere = pl.BlockSpec(memory_space=pl.ANY)
    vector = pl.BlockSpec(memory_space=pltpu.VMEM)
    scalar = pl.BlockSpec(memory_space=pltpu.SMEM)
    return pl.pallas_call(
        place_kernel,
        out_shape=jax.ShapeDtypeStruct((G_DEV, nodes, hidden), jnp.bfloat16),
        in_specs=[scalar, scalar, anywhere] + [vector] * 6,
        out_specs=anywhere,
        scratch_shapes=[
            pltpu.VMEM((G_DEV, nodes, hidden), jnp.bfloat16),
            pltpu.VMEM((G_DEV, nodes, hidden), jnp.bfloat16),
            pltpu.SemaphoreType.DMA((G_DEV // MLP,)),
            pltpu.SemaphoreType.DMA((G_DEV // MLP,)),
        ],
        compiler_params=pltpu.CompilerParams(vmem_limit_bytes=VMEM_BYTES),
        cost_estimate=mlp_cost(G_DEV * nodes, hidden),
        name="place",
    )(chips, counts, arrived, *weights)


def body(
    node_features,
    node_counts,
    edge_list,
    readout_ids,
    live_graphs,
    self_weight,
    w_first,
    b_first,
    w_second,
    b_second,
    w_third,
    b_third,
):
    weights = (
        w_first,
        b_first[None, :],
        w_second,
        b_second[None, :],
        w_third,
        b_third[None, :],
    )
    devices = lax.axis_size(ROW_COL)
    capacity, nodes, hidden = node_features.shape
    me = lax.axis_index(ROW_COL)
    core = lax.axis_index("col_2")
    chip = lax.axis_index(CHIP)

    par_features = lax.ppermute(node_features, "col_2", SWAP)
    par_edges = lax.ppermute(edge_list, "col_2", SWAP)
    info = jnp.concatenate([live_graphs, node_counts, readout_ids])
    table = lax.all_to_all(
        jnp.broadcast_to(info[None], (devices, info.shape[0])), ROW_COL, 0, 0, tiled=True
    )
    live = table[:, 0]

    device = lax.broadcasted_iota(jnp.int32, (4, devices), 1)
    part = lax.broadcasted_iota(jnp.int32, (4, devices), 0)
    ahead = (part == 1) & (device < 2 * chip)
    mine = (part >= 2) & (device == 2 * chip + part - 2)
    own = (part == 0) & (device < core)
    place = masked_sum(ahead | mine | own, jnp.where(own, 1, live[None, :]), 1)

    blended = blended_slots(
        node_features, par_features, edge_list, par_edges, place, self_weight
    )
    arrived = lax.all_to_all(blended, CHIP, split_axis=0, concat_axis=0, tiled=True)

    offset, live_a, live_b = place[1], place[2], place[3]
    slot = lax.broadcasted_iota(jnp.int32, (devices // 2,), 0)
    number = (2 * slot + core - offset) & (devices - 1)
    filled = number < live_a + live_b
    picked = jnp.where(number >= live_a, capacity + number - live_a, number)
    pair = lax.dynamic_slice_in_dim(table, 2 * chip, 2, 0)
    spot = lax.broadcasted_iota(jnp.int32, (devices // 2, 2 * capacity), 1) == picked[:, None]
    spot = spot & filled[:, None]
    slot_counts = masked_sum(spot, pair[:, 1 : 1 + capacity].reshape(1, -1), 1)
    slot_ids = masked_sum(spot, pair[:, 1 + capacity :].reshape(1, -1), 1)
    slot_ids = jnp.where(filled, slot_ids, -1)
    pooled = pooled_slots(blended, slot_counts, weights)
    groups = READ_DEV * devices
    id_keys = lax.broadcasted_iota(jnp.int32, (groups, slot_ids.shape[0]), 0)
    members = (id_keys == slot_ids[None, :]).astype(jnp.float32)
    terms = jnp.dot(
        members, pooled, precision=lax.Precision.HIGHEST, preferred_element_type=jnp.float32
    )
    terms = terms.reshape(devices // 2, 2, READ_DEV, hidden)
    kept = lax.dynamic_index_in_dim(terms, core, 1, keepdims=False)
    sent = lax.dynamic_index_in_dim(terms, 1 - core, 1, keepdims=False).astype(jnp.bfloat16)
    both = kept + lax.ppermute(sent, "col_2", SWAP).astype(jnp.float32)
    both, arrived = lax.optimization_barrier((both.astype(jnp.bfloat16), arrived))
    sums = lax.all_to_all(both, CHIP, split_axis=0, concat_axis=0, tiled=True)
    readout = jnp.sum(sums.astype(jnp.float32), axis=0)

    order = lax.broadcasted_iota(jnp.int32, (G_DEV, 1), 0) * devices + me
    shape = (devices, devices)
    before = lax.broadcasted_iota(jnp.int32, shape, 1) <= lax.broadcasted_iota(jnp.int32, shape, 0)
    upto = masked_sum(before, live[None, :], 1)
    passed = upto[None, :] <= order
    source = jnp.sum(passed.astype(jnp.int32), axis=1)
    start = jnp.max(jnp.where(passed, upto[None, :], 0), axis=1)
    source_idx = order[:, 0] - start
    every = lax.broadcasted_iota(jnp.int32, (devices,), 0)
    hit = (every[None, :, None] == source[:, None, None]) & (
        lax.broadcasted_iota(jnp.int32, (1, 1, capacity), 2) == source_idx[:, None, None]
    )
    counts = jnp.sum(jnp.where(hit, table[None, :, 1 : 1 + capacity], 0), axis=(1, 2))
    node_out = placed_nodes(arrived, source >> 1, counts, weights)
    return (node_out, readout)


def solution(mesh):
    split = Mesh(
        mesh.devices.reshape(mesh.shape["row"], 4, 4, 2), ("row", "col_0", "col_1", "col_2")
    )
    return jax.shard_map(
        body,
        mesh=split,
        in_specs=(
            P(ROW_COL, None, None),
            P(ROW_COL),
            P(ROW_COL, None, None),
            P(ROW_COL),
            P(ROW_COL),
            P(),
            P(),
            P(),
            P(),
            P(),
            P(),
            P(),
        ),
        out_specs=(P(ROW_COL, None, None), P(ROW_COL, None)),
        check_vma=False,
    )
```

```python
import jax
import jax.numpy as jnp
from jax import lax
from jax.experimental import pallas as pl
from jax.experimental.pallas import tpu as pltpu
from jax.sharding import Mesh
from jax.sharding import PartitionSpec as P

G_DEV = 32
READ_DEV = 8
ROW_COL = ("row", "col_0", "col_1", "col_2")
CHIP = ("row", "col_0", "col_1")
SWAP = [(0, 1), (1, 0)]
PACK_BITS = 3
PACK = 1 << PACK_BITS
POOL = 8
MLP_BITS = 2
HEAD_ROWS = 112
TAIL_GRAPHS = 16
MLP = 1 << MLP_BITS
VMEM_BYTES = 58 * 1024 * 1024
FINISH_BYTES = 24 * 1024 * 1024


def masked_sum(keep, values, axis):
    return jnp.sum(jnp.where(keep, values, 0), axis=axis)


def blend_kernel(
    where, scale, own, par, own_edges, par_edges, head, tail, taken, made, taken_sem, made_sem
):
    core, offset, live_a, live_b = where[0], where[1], where[2], where[3]
    count, nodes, _ = taken.shape
    wrap = 2 * count - 1
    node_index = lax.broadcasted_iota(jnp.int32, (nodes, own_edges.shape[-1]), 0)

    def source_of(slot):
        number = (2 * slot + core - offset) & wrap
        filled = number < live_a + live_b
        from_b = number >= live_a
        index = jnp.where(filled, jnp.where(from_b, number - live_a, number), slot)
        return index, jnp.logical_xor(from_b, core == 1)

    @pl.loop(0, count)
    def _(slot):
        index, from_par = source_of(slot)
        sem = taken_sem.at[slot >> PACK_BITS]

        @pl.when(from_par)
        def _():
            pltpu.make_async_copy(par.at[index], taken.at[slot], sem).start()

        @pl.when(jnp.logical_not(from_par))
        def _():
            pltpu.make_async_copy(own.at[index], taken.at[slot], sem).start()

    cuts = ((head, pl.ds(0, HEAD_ROWS)), (tail, pl.ds(HEAD_ROWS, nodes - HEAD_ROWS)))

    def put(group, which):
        rows = pl.ds(group * PACK, PACK)
        out, cut = cuts[which]
        return pltpu.make_async_copy(made.at[rows, cut], out.at[rows], made_sem.at[which, group])

    @pl.loop(0, count // PACK)
    def _(group):
        pltpu.make_async_copy(
            own.at[pl.ds(0, PACK)], taken.at[pl.ds(group * PACK, PACK)], taken_sem.at[group]
        ).wait()
        slots = [group * PACK + lane for lane in range(PACK)]
        sources, targets = [], []
        for slot in slots:
            index, from_par = source_of(slot)
            edges = jnp.where(from_par, par_edges[index], own_edges[index])
            sources.append((node_index == edges[0:1, :]).astype(jnp.bfloat16))
            targets.append((node_index == edges[1:2, :]).astype(jnp.bfloat16))
        adjacency = [
            lax.dot_general(t, s, (((1,), (1,)), ((), ())), preferred_element_type=jnp.float32)
            for t, s in zip(targets, sources)
        ]
        features = [taken[slot] for slot in slots]
        neighbours = [
            jnp.dot(a.astype(jnp.bfloat16), f, preferred_element_type=jnp.float32)
            for a, f in zip(adjacency, features)
        ]
        for slot, f, n in zip(slots, features, neighbours):
            made[slot] = (scale[0] * f.astype(jnp.float32) + n).astype(jnp.bfloat16)
        put(group, 0).start()
        put(group, 1).start()

    @pl.loop(0, count // PACK)
    def _(group):
        put(group, 0).wait()
        put(group, 1).wait()


def blended_slots(own, par, own_edges, par_edges, where, scale):
    count, nodes, hidden = own.shape
    anywhere = pl.BlockSpec(memory_space=pl.ANY)
    vector = pl.BlockSpec(memory_space=pltpu.VMEM)
    scalar = pl.BlockSpec(memory_space=pltpu.SMEM)
    return pl.pallas_call(
        blend_kernel,
        out_shape=[
            jax.ShapeDtypeStruct((count, rows, hidden), jnp.bfloat16)
            for rows in (HEAD_ROWS, nodes - HEAD_ROWS)
        ],
        in_specs=[scalar, scalar, anywhere, anywhere, vector, vector],
        out_specs=[anywhere, anywhere],
        scratch_shapes=[
            pltpu.VMEM((count, nodes, hidden), jnp.bfloat16),
            pltpu.VMEM((count, nodes, hidden), jnp.bfloat16),
            pltpu.SemaphoreType.DMA((count // PACK,)),
            pltpu.SemaphoreType.DMA((2, count // PACK)),
        ],
        compiler_params=pltpu.CompilerParams(vmem_limit_bytes=VMEM_BYTES),
        cost_estimate=pl.CostEstimate(
            flops=2 * count * nodes * nodes * (own_edges.shape[-1] + hidden),
            bytes_accessed=4 * count * nodes * hidden,
            transcendentals=0,
        ),
        name="blend",
    )(where, scale, own, par, own_edges, par_edges)


def perceptron(rows, weights):
    w_first, b_first, w_second, b_second, w_third, b_third = weights
    for w, b in ((w_first, b_first), (w_second, b_second)):
        total = jnp.dot(rows, w[...], preferred_element_type=jnp.float32) + b[...]
        rows = jnp.maximum(total, 0.0).astype(jnp.bfloat16)
    return jnp.dot(rows, w_third[...], preferred_element_type=jnp.float32) + b_third[...]


def weight_specs(weights):
    return [pl.BlockSpec(w.shape, lambda i, *tables: (0, 0)) for w in weights]


def mlp_cost(rows, hidden):
    return pl.CostEstimate(
        flops=6 * rows * hidden * hidden, bytes_accessed=4 * rows * hidden, transcendentals=0
    )


def pool_kernel(counts, head_ref, tail_ref, *refs):
    weights, out = refs[:6], refs[6]
    step = pl.program_id(0)
    many, head, hidden = head_ref.shape
    tail = tail_ref.shape[1]
    rows = jnp.concatenate(
        [head_ref[...].reshape(many * head, hidden), tail_ref[...].reshape(many * tail, hidden)],
        axis=0,
    )
    result = perceptron(rows, weights)
    for lane in range(many):
        count = counts[step * many + lane]
        total = jnp.zeros((1, hidden), jnp.float32)
        for first, start, size in ((0, lane * head, head), (head, many * head + lane * tail, tail)):
            node_index = first + lax.broadcasted_iota(jnp.int32, (size, 1), 0)
            kept = jnp.where(node_index < count, result[start : start + size], 0.0)
            kept = kept.astype(jnp.bfloat16).astype(jnp.float32)
            total = total + jnp.sum(kept, axis=0, keepdims=True)
        out[lane : lane + 1, :] = total / jnp.maximum(count, 1).astype(jnp.float32)


def pooled_slots(heads, tails, counts, weights):
    count, head, hidden = heads.shape
    tail = tails.shape[1]
    return pl.pallas_call(
        pool_kernel,
        out_shape=jax.ShapeDtypeStruct((count, hidden), jnp.float32),
        grid_spec=pltpu.PrefetchScalarGridSpec(
            num_scalar_prefetch=1,
            grid=(count // POOL,),
            in_specs=[
                pl.BlockSpec((POOL, head, hidden), lambda i, *tables: (i, 0, 0)),
                pl.BlockSpec((POOL, tail, hidden), lambda i, *tables: (i, 0, 0)),
            ]
            + weight_specs(weights),
            out_specs=pl.BlockSpec((POOL, hidden), lambda i, *tables: (i, 0)),
        ),
        compiler_params=pltpu.CompilerParams(dimension_semantics=("arbitrary",)),
        cost_estimate=mlp_cost(count * (head + tail), hidden),
        name="pool",
    )(counts, heads, tails, *weights)


def place_kernel(chips, counts, arrived, *refs):
    weights, out, taken, made, taken_sem, made_sem = refs[:6], *refs[6:]
    count, nodes, hidden = taken.shape

    @pl.loop(0, count)
    def _(slot):
        pltpu.make_async_copy(
            arrived.at[chips[slot]], taken.at[slot], taken_sem.at[slot >> MLP_BITS]
        ).start()

    def put(group):
        rows = pl.ds(group * MLP, MLP)
        return pltpu.make_async_copy(
            made.at[rows], out.at[rows, pl.ds(0, nodes)], made_sem.at[group]
        )

    node_index = lax.broadcasted_iota(jnp.int32, (nodes, 1), 0)

    @pl.loop(0, count // MLP)
    def _(group):
        rows = pl.ds(group * MLP, MLP)
        pltpu.make_async_copy(
            arrived.at[pl.ds(0, MLP)], taken.at[rows], taken_sem.at[group]
        ).wait()
        result = perceptron(taken[rows].reshape(MLP * nodes, hidden), weights)
        for lane in range(MLP):
            slot = group * MLP + lane
            part = result[lane * nodes : (lane + 1) * nodes]
            made[slot] = jnp.where(node_index < counts[slot], part, 0.0).astype(jnp.bfloat16)
        put(group).start()

    @pl.loop(0, count // MLP)
    def _(group):
        put(group).wait()


def placed_heads(arrived, chips, counts, weights, nodes):
    _, head, hidden = arrived.shape
    anywhere = pl.BlockSpec(memory_space=pl.ANY)
    vector = pl.BlockSpec(memory_space=pltpu.VMEM)
    scalar = pl.BlockSpec(memory_space=pltpu.SMEM)
    return pl.pallas_call(
        place_kernel,
        out_shape=jax.ShapeDtypeStruct((G_DEV, nodes, hidden), jnp.bfloat16),
        in_specs=[scalar, scalar, anywhere] + [vector] * 6,
        out_specs=anywhere,
        scratch_shapes=[
            pltpu.VMEM((G_DEV, head, hidden), jnp.bfloat16),
            pltpu.VMEM((G_DEV, head, hidden), jnp.bfloat16),
            pltpu.SemaphoreType.DMA((G_DEV // MLP,)),
            pltpu.SemaphoreType.DMA((G_DEV // MLP,)),
        ],
        compiler_params=pltpu.CompilerParams(vmem_limit_bytes=VMEM_BYTES),
        cost_estimate=mlp_cost(G_DEV * head, hidden),
        name="place",
    )(chips, counts, arrived, *weights)


def finish_kernel(chips, counts, arrived, *refs):
    weights, (_, out, readout, made, made_sem) = refs[:6], refs[6:]
    count, tail, hidden = made.shape
    nodes = out.shape[1]

    def put(group):
        rows = pl.ds(group * TAIL_GRAPHS, TAIL_GRAPHS)
        return pltpu.make_async_copy(
            made.at[rows], out.at[rows, pl.ds(nodes - tail, tail)], made_sem.at[group]
        )

    node_index = nodes - tail + lax.broadcasted_iota(jnp.int32, (tail, 1), 0)
    for group in range(count // TAIL_GRAPHS):
        slots = [group * TAIL_GRAPHS + lane for lane in range(TAIL_GRAPHS)]
        rows = jnp.concatenate([arrived[chips[slot], :tail] for slot in slots], axis=0)
        result = perceptron(rows, weights)
        for lane, slot in enumerate(slots):
            part = result[lane * tail : (lane + 1) * tail]
            made[slot] = jnp.where(node_index < counts[slot], part, 0.0).astype(jnp.bfloat16)
        put(group).start()
    readout[...] = jnp.sum(arrived[:, tail:].astype(jnp.float32), axis=0)
    for group in range(count // TAIL_GRAPHS):
        put(group).wait()


def finished(node_out, arrived, chips, counts, weights):
    count, nodes, hidden = node_out.shape
    tail = arrived.shape[1] - READ_DEV
    anywhere = pl.BlockSpec(memory_space=pl.ANY)
    vector = pl.BlockSpec(memory_space=pltpu.VMEM)
    scalar = pl.BlockSpec(memory_space=pltpu.SMEM)
    return pl.pallas_call(
        finish_kernel,
        out_shape=[
            jax.ShapeDtypeStruct(node_out.shape, jnp.bfloat16),
            jax.ShapeDtypeStruct((READ_DEV, hidden), jnp.float32),
        ],
        in_specs=[scalar, scalar, vector] + [vector] * 6 + [anywhere],
        out_specs=[anywhere, vector],
        scratch_shapes=[
            pltpu.VMEM((count, tail, hidden), jnp.bfloat16),
            pltpu.SemaphoreType.DMA((count // TAIL_GRAPHS,)),
        ],
        input_output_aliases={9: 0},
        compiler_params=pltpu.CompilerParams(vmem_limit_bytes=FINISH_BYTES),
        cost_estimate=mlp_cost(count * tail, hidden),
        name="finish",
    )(chips, counts, arrived, *weights, node_out)


def body(
    node_features,
    node_counts,
    edge_list,
    readout_ids,
    live_graphs,
    self_weight,
    w_first,
    b_first,
    w_second,
    b_second,
    w_third,
    b_third,
):
    weights = (
        w_first,
        b_first[None, :],
        w_second,
        b_second[None, :],
        w_third,
        b_third[None, :],
    )
    devices = lax.axis_size(ROW_COL)
    capacity, nodes, hidden = node_features.shape
    me = lax.axis_index(ROW_COL)
    core = lax.axis_index("col_2")
    chip = lax.axis_index(CHIP)

    par_features = lax.ppermute(node_features, "col_2", SWAP)
    par_edges = lax.ppermute(edge_list, "col_2", SWAP)
    info = jnp.concatenate([live_graphs, node_counts, readout_ids])
    table = lax.all_to_all(
        jnp.broadcast_to(info[None], (devices, info.shape[0])), ROW_COL, 0, 0, tiled=True
    )
    live = table[:, 0]

    device = lax.broadcasted_iota(jnp.int32, (4, devices), 1)
    part = lax.broadcasted_iota(jnp.int32, (4, devices), 0)
    ahead = (part == 1) & (device < 2 * chip)
    mine = (part >= 2) & (device == 2 * chip + part - 2)
    own = (part == 0) & (device < core)
    place = masked_sum(ahead | mine | own, jnp.where(own, 1, live[None, :]), 1)

    heads, tails = blended_slots(
        node_features, par_features, edge_list, par_edges, place, self_weight
    )
    arrived = lax.all_to_all(heads, CHIP, split_axis=0, concat_axis=0, tiled=True)

    offset, live_a, live_b = place[1], place[2], place[3]
    slot = lax.broadcasted_iota(jnp.int32, (devices // 2,), 0)
    number = (2 * slot + core - offset) & (devices - 1)
    filled = number < live_a + live_b
    picked = jnp.where(number >= live_a, capacity + number - live_a, number)
    pair = lax.dynamic_slice_in_dim(table, 2 * chip, 2, 0)
    spot = lax.broadcasted_iota(jnp.int32, (devices // 2, 2 * capacity), 1) == picked[:, None]
    spot = spot & filled[:, None]
    slot_counts = masked_sum(spot, pair[:, 1 : 1 + capacity].reshape(1, -1), 1)
    slot_ids = masked_sum(spot, pair[:, 1 + capacity :].reshape(1, -1), 1)
    slot_ids = jnp.where(filled, slot_ids, -1)
    pooled = pooled_slots(heads, tails, slot_counts, weights)
    groups = READ_DEV * devices
    id_keys = lax.broadcasted_iota(jnp.int32, (groups, slot_ids.shape[0]), 0)
    members = (id_keys == slot_ids[None, :]).astype(jnp.float32)
    terms = jnp.dot(
        members, pooled, precision=lax.Precision.HIGHEST, preferred_element_type=jnp.float32
    )
    terms = terms.reshape(devices // 2, 2, READ_DEV, hidden)
    kept = lax.dynamic_index_in_dim(terms, core, 1, keepdims=False)
    sent = lax.dynamic_index_in_dim(terms, 1 - core, 1, keepdims=False).astype(jnp.bfloat16)
    both = kept + lax.ppermute(sent, "col_2", SWAP).astype(jnp.float32)
    rest = jnp.concatenate([tails, both.astype(jnp.bfloat16)], axis=1)
    rest, arrived = lax.optimization_barrier((rest, arrived))
    arrived_rest = lax.all_to_all(rest, CHIP, split_axis=0, concat_axis=0, tiled=True)

    order = lax.broadcasted_iota(jnp.int32, (G_DEV, 1), 0) * devices + me
    shape = (devices, devices)
    before = lax.broadcasted_iota(jnp.int32, shape, 1) <= lax.broadcasted_iota(jnp.int32, shape, 0)
    upto = masked_sum(before, live[None, :], 1)
    passed = upto[None, :] <= order
    source = jnp.sum(passed.astype(jnp.int32), axis=1)
    start = jnp.max(jnp.where(passed, upto[None, :], 0), axis=1)
    source_idx = order[:, 0] - start
    every = lax.broadcasted_iota(jnp.int32, (devices,), 0)
    hit = (every[None, :, None] == source[:, None, None]) & (
        lax.broadcasted_iota(jnp.int32, (1, 1, capacity), 2) == source_idx[:, None, None]
    )
    counts = jnp.sum(jnp.where(hit, table[None, :, 1 : 1 + capacity], 0), axis=(1, 2))
    chips = source >> 1
    node_out = placed_heads(arrived, chips, counts, weights, nodes)
    return tuple(finished(node_out, arrived_rest, chips, counts, weights))


def solution(mesh):
    split = Mesh(
        mesh.devices.reshape(mesh.shape["row"], 4, 4, 2), ("row", "col_0", "col_1", "col_2")
    )
    return jax.shard_map(
        body,
        mesh=split,
        in_specs=(
            P(ROW_COL, None, None),
            P(ROW_COL),
            P(ROW_COL, None, None),
            P(ROW_COL),
            P(ROW_COL),
            P(),
            P(),
            P(),
            P(),
            P(),
            P(),
            P(),
        ),
        out_specs=(P(ROW_COL, None, None), P(ROW_COL, None)),
        check_vma=False,
    )
```

```python
import jax
import jax.numpy as jnp
from jax import lax
from jax.experimental import pallas as pl
from jax.experimental.pallas import tpu as pltpu
from jax.sharding import Mesh
from jax.sharding import PartitionSpec as P

G_DEV = 32
READ_DEV = 8
ROW_COL = ("row", "col_0", "col_1", "col_2")
CHIP = ("row", "col_0", "col_1")
SWAP = [(0, 1), (1, 0)]
PACK_BITS = 3
PACK = 1 << PACK_BITS
POOL = 8
MLP_BITS = 3
HEAD_ROWS = 80
TAIL_BITS = 3
TAIL_GRAPHS = 1 << TAIL_BITS
MLP = 1 << MLP_BITS
VMEM_BYTES = 59 * 1024 * 1024


def masked_sum(keep, values, axis):
    return jnp.sum(jnp.where(keep, values, 0), axis=axis)


def blend_kernel(
    where, scale, own, par, own_edges, par_edges, head, tail, taken, made, taken_sem, made_sem
):
    core, offset, live_a, live_b = where[0], where[1], where[2], where[3]
    count, nodes, _ = taken.shape
    wrap = 2 * count - 1
    node_index = lax.broadcasted_iota(jnp.int32, (nodes, own_edges.shape[-1]), 0)

    def source_of(slot):
        number = (2 * slot + core - offset) & wrap
        filled = number < live_a + live_b
        from_b = number >= live_a
        index = jnp.where(filled, jnp.where(from_b, number - live_a, number), slot)
        return index, jnp.logical_xor(from_b, core == 1)

    @pl.loop(0, count)
    def _(slot):
        index, from_par = source_of(slot)
        sem = taken_sem.at[slot >> PACK_BITS]

        @pl.when(from_par)
        def _():
            pltpu.make_async_copy(par.at[index], taken.at[slot], sem).start()

        @pl.when(jnp.logical_not(from_par))
        def _():
            pltpu.make_async_copy(own.at[index], taken.at[slot], sem).start()

    cuts = ((head, pl.ds(0, HEAD_ROWS)), (tail, pl.ds(HEAD_ROWS, nodes - HEAD_ROWS)))

    def put(group, which):
        rows = pl.ds(group * PACK, PACK)
        out, cut = cuts[which]
        return pltpu.make_async_copy(made.at[rows, cut], out.at[rows], made_sem.at[which, group])

    @pl.loop(0, count // PACK)
    def _(group):
        pltpu.make_async_copy(
            own.at[pl.ds(0, PACK)], taken.at[pl.ds(group * PACK, PACK)], taken_sem.at[group]
        ).wait()
        slots = [group * PACK + lane for lane in range(PACK)]
        sources, targets = [], []
        for slot in slots:
            index, from_par = source_of(slot)
            edges = jnp.where(from_par, par_edges[index], own_edges[index])
            sources.append((node_index == edges[0:1, :]).astype(jnp.bfloat16))
            targets.append((node_index == edges[1:2, :]).astype(jnp.bfloat16))
        adjacency = [
            lax.dot_general(t, s, (((1,), (1,)), ((), ())), preferred_element_type=jnp.float32)
            for t, s in zip(targets, sources)
        ]
        features = [taken[slot] for slot in slots]
        neighbours = [
            jnp.dot(a.astype(jnp.bfloat16), f, preferred_element_type=jnp.float32)
            for a, f in zip(adjacency, features)
        ]
        for slot, f, n in zip(slots, features, neighbours):
            made[slot] = (scale[0] * f.astype(jnp.float32) + n).astype(jnp.bfloat16)
        put(group, 0).start()
        put(group, 1).start()

    @pl.loop(0, count // PACK)
    def _(group):
        put(group, 0).wait()
        put(group, 1).wait()


def blended_slots(own, par, own_edges, par_edges, where, scale):
    count, nodes, hidden = own.shape
    anywhere = pl.BlockSpec(memory_space=pl.ANY)
    vector = pl.BlockSpec(memory_space=pltpu.VMEM)
    scalar = pl.BlockSpec(memory_space=pltpu.SMEM)
    return pl.pallas_call(
        blend_kernel,
        out_shape=[
            jax.ShapeDtypeStruct((count, rows, hidden), jnp.bfloat16)
            for rows in (HEAD_ROWS, nodes - HEAD_ROWS)
        ],
        in_specs=[scalar, scalar, anywhere, anywhere, vector, vector],
        out_specs=[anywhere, anywhere],
        scratch_shapes=[
            pltpu.VMEM((count, nodes, hidden), jnp.bfloat16),
            pltpu.VMEM((count, nodes, hidden), jnp.bfloat16),
            pltpu.SemaphoreType.DMA((count // PACK,)),
            pltpu.SemaphoreType.DMA((2, count // PACK)),
        ],
        compiler_params=pltpu.CompilerParams(vmem_limit_bytes=VMEM_BYTES),
        cost_estimate=pl.CostEstimate(
            flops=2 * count * nodes * nodes * (own_edges.shape[-1] + hidden),
            bytes_accessed=4 * count * nodes * hidden,
            transcendentals=0,
        ),
        name="blend",
    )(where, scale, own, par, own_edges, par_edges)


def perceptron(rows, weights):
    w_first, b_first, w_second, b_second, w_third, b_third = weights
    for w, b in ((w_first, b_first), (w_second, b_second)):
        total = jnp.dot(rows, w[...], preferred_element_type=jnp.float32) + b[...]
        rows = jnp.maximum(total, 0.0).astype(jnp.bfloat16)
    return jnp.dot(rows, w_third[...], preferred_element_type=jnp.float32) + b_third[...]


def weight_specs(weights):
    return [pl.BlockSpec(w.shape, lambda i, *tables: (0, 0)) for w in weights]


def mlp_cost(rows, hidden):
    return pl.CostEstimate(
        flops=6 * rows * hidden * hidden, bytes_accessed=4 * rows * hidden, transcendentals=0
    )


def pool_kernel(counts, head_ref, tail_ref, *refs):
    weights, out = refs[:6], refs[6]
    step = pl.program_id(0)
    many, head, hidden = head_ref.shape
    tail = tail_ref.shape[1]
    rows = jnp.concatenate(
        [head_ref[...].reshape(many * head, hidden), tail_ref[...].reshape(many * tail, hidden)],
        axis=0,
    )
    result = perceptron(rows, weights)
    for lane in range(many):
        count = counts[step * many + lane]
        total = jnp.zeros((1, hidden), jnp.float32)
        for first, start, size in ((0, lane * head, head), (head, many * head + lane * tail, tail)):
            node_index = first + lax.broadcasted_iota(jnp.int32, (size, 1), 0)
            kept = jnp.where(node_index < count, result[start : start + size], 0.0)
            kept = kept.astype(jnp.bfloat16).astype(jnp.float32)
            total = total + jnp.sum(kept, axis=0, keepdims=True)
        out[lane : lane + 1, :] = total / jnp.maximum(count, 1).astype(jnp.float32)


def pooled_slots(heads, tails, counts, weights):
    count, head, hidden = heads.shape
    tail = tails.shape[1]
    return pl.pallas_call(
        pool_kernel,
        out_shape=jax.ShapeDtypeStruct((count, hidden), jnp.float32),
        grid_spec=pltpu.PrefetchScalarGridSpec(
            num_scalar_prefetch=1,
            grid=(count // POOL,),
            in_specs=[
                pl.BlockSpec((POOL, head, hidden), lambda i, *tables: (i, 0, 0)),
                pl.BlockSpec((POOL, tail, hidden), lambda i, *tables: (i, 0, 0)),
            ]
            + weight_specs(weights),
            out_specs=pl.BlockSpec((POOL, hidden), lambda i, *tables: (i, 0)),
        ),
        compiler_params=pltpu.CompilerParams(dimension_semantics=("arbitrary",)),
        cost_estimate=mlp_cost(count * (head + tail), hidden),
        name="pool",
    )(counts, heads, tails, *weights)


def place_kernel(chips, counts, arrived, *refs):
    weights, out, taken, made, taken_sem, made_sem = refs[:6], *refs[6:]
    count, nodes, hidden = taken.shape

    @pl.loop(0, count)
    def _(slot):
        pltpu.make_async_copy(
            arrived.at[chips[slot]], taken.at[slot], taken_sem.at[slot >> MLP_BITS]
        ).start()

    def put(group):
        rows = pl.ds(group * MLP, MLP)
        return pltpu.make_async_copy(
            made.at[rows], out.at[rows, pl.ds(0, nodes)], made_sem.at[group]
        )

    node_index = lax.broadcasted_iota(jnp.int32, (nodes, 1), 0)

    @pl.loop(0, count // MLP)
    def _(group):
        rows = pl.ds(group * MLP, MLP)
        pltpu.make_async_copy(
            arrived.at[pl.ds(0, MLP)], taken.at[rows], taken_sem.at[group]
        ).wait()
        result = perceptron(taken[rows].reshape(MLP * nodes, hidden), weights)
        for lane in range(MLP):
            slot = group * MLP + lane
            part = result[lane * nodes : (lane + 1) * nodes]
            made[slot] = jnp.where(node_index < counts[slot], part, 0.0).astype(jnp.bfloat16)
        put(group).start()

    @pl.loop(0, count // MLP)
    def _(group):
        put(group).wait()


def placed_heads(arrived, chips, counts, weights, nodes):
    _, head, hidden = arrived.shape
    anywhere = pl.BlockSpec(memory_space=pl.ANY)
    vector = pl.BlockSpec(memory_space=pltpu.VMEM)
    scalar = pl.BlockSpec(memory_space=pltpu.SMEM)
    return pl.pallas_call(
        place_kernel,
        out_shape=jax.ShapeDtypeStruct((G_DEV, nodes, hidden), jnp.bfloat16),
        in_specs=[scalar, scalar, anywhere] + [vector] * 6,
        out_specs=anywhere,
        scratch_shapes=[
            pltpu.VMEM((G_DEV, head, hidden), jnp.bfloat16),
            pltpu.VMEM((G_DEV, head, hidden), jnp.bfloat16),
            pltpu.SemaphoreType.DMA((G_DEV // MLP,)),
            pltpu.SemaphoreType.DMA((G_DEV // MLP,)),
        ],
        compiler_params=pltpu.CompilerParams(vmem_limit_bytes=VMEM_BYTES),
        cost_estimate=mlp_cost(G_DEV * head, hidden),
        name="place",
    )(chips, counts, arrived, *weights)


def finish_kernel(chips, counts, arrived, *refs):
    weights, refs = refs[:6], refs[7:]
    out, readout, taken, made, terms, taken_sem, made_sem, terms_sem = refs
    count, tail, hidden = taken.shape
    nodes = out.shape[1]
    own_rows = pl.ds(0, tail)

    @pl.loop(0, count)
    def _(slot):
        pltpu.make_async_copy(
            arrived.at[chips[slot], own_rows], taken.at[slot], taken_sem.at[slot >> TAIL_BITS]
        ).start()

    summed = pltpu.make_async_copy(arrived.at[:, pl.ds(tail, READ_DEV)], terms, terms_sem)
    summed.start()

    def put(group):
        rows = pl.ds(group * TAIL_GRAPHS, TAIL_GRAPHS)
        return pltpu.make_async_copy(
            made.at[rows], out.at[rows, pl.ds(nodes - tail, tail)], made_sem.at[group]
        )

    node_index = nodes - tail + lax.broadcasted_iota(jnp.int32, (tail, 1), 0)

    @pl.loop(0, count // TAIL_GRAPHS)
    def _(group):
        rows = pl.ds(group * TAIL_GRAPHS, TAIL_GRAPHS)
        pltpu.make_async_copy(
            arrived.at[pl.ds(0, TAIL_GRAPHS), own_rows], taken.at[rows], taken_sem.at[group]
        ).wait()
        result = perceptron(taken[rows].reshape(TAIL_GRAPHS * tail, hidden), weights)
        for lane in range(TAIL_GRAPHS):
            slot = group * TAIL_GRAPHS + lane
            part = result[lane * tail : (lane + 1) * tail]
            made[slot] = jnp.where(node_index < counts[slot], part, 0.0).astype(jnp.bfloat16)
        put(group).start()

    summed.wait()
    readout[...] = jnp.sum(terms[...].astype(jnp.float32), axis=0)

    @pl.loop(0, count // TAIL_GRAPHS)
    def _(group):
        put(group).wait()


def finished(node_out, arrived, chips, counts, weights):
    count, nodes, hidden = node_out.shape
    tail = arrived.shape[1] - READ_DEV
    anywhere = pl.BlockSpec(memory_space=pl.ANY)
    vector = pl.BlockSpec(memory_space=pltpu.VMEM)
    scalar = pl.BlockSpec(memory_space=pltpu.SMEM)
    return pl.pallas_call(
        finish_kernel,
        out_shape=[
            jax.ShapeDtypeStruct(node_out.shape, jnp.bfloat16),
            jax.ShapeDtypeStruct((READ_DEV, hidden), jnp.float32),
        ],
        in_specs=[scalar, scalar, anywhere] + [vector] * 6 + [anywhere],
        out_specs=[anywhere, vector],
        scratch_shapes=[
            pltpu.VMEM((count, tail, hidden), jnp.bfloat16),
            pltpu.VMEM((count, tail, hidden), jnp.bfloat16),
            pltpu.VMEM((arrived.shape[0], READ_DEV, hidden), jnp.bfloat16),
            pltpu.SemaphoreType.DMA((count // TAIL_GRAPHS,)),
            pltpu.SemaphoreType.DMA((count // TAIL_GRAPHS,)),
            pltpu.SemaphoreType.DMA,
        ],
        input_output_aliases={9: 0},
        compiler_params=pltpu.CompilerParams(vmem_limit_bytes=VMEM_BYTES),
        cost_estimate=mlp_cost(count * tail, hidden),
        name="finish",
    )(chips, counts, arrived, *weights, node_out)


def body(
    node_features,
    node_counts,
    edge_list,
    readout_ids,
    live_graphs,
    self_weight,
    w_first,
    b_first,
    w_second,
    b_second,
    w_third,
    b_third,
):
    weights = (
        w_first,
        b_first[None, :],
        w_second,
        b_second[None, :],
        w_third,
        b_third[None, :],
    )
    devices = lax.axis_size(ROW_COL)
    capacity, nodes, hidden = node_features.shape
    me = lax.axis_index(ROW_COL)
    core = lax.axis_index("col_2")
    chip = lax.axis_index(CHIP)

    par_features = lax.ppermute(node_features, "col_2", SWAP)
    par_edges = lax.ppermute(edge_list, "col_2", SWAP)
    info = jnp.concatenate([live_graphs, node_counts, readout_ids])
    table = lax.all_to_all(
        jnp.broadcast_to(info[None], (devices, info.shape[0])), ROW_COL, 0, 0, tiled=True
    )
    live = table[:, 0]

    device = lax.broadcasted_iota(jnp.int32, (4, devices), 1)
    part = lax.broadcasted_iota(jnp.int32, (4, devices), 0)
    ahead = (part == 1) & (device < 2 * chip)
    mine = (part >= 2) & (device == 2 * chip + part - 2)
    own = (part == 0) & (device < core)
    place = masked_sum(ahead | mine | own, jnp.where(own, 1, live[None, :]), 1)

    heads, tails = blended_slots(
        node_features, par_features, edge_list, par_edges, place, self_weight
    )
    arrived = lax.all_to_all(heads, CHIP, split_axis=0, concat_axis=0, tiled=True)

    offset, live_a, live_b = place[1], place[2], place[3]
    slot = lax.broadcasted_iota(jnp.int32, (devices // 2,), 0)
    number = (2 * slot + core - offset) & (devices - 1)
    filled = number < live_a + live_b
    picked = jnp.where(number >= live_a, capacity + number - live_a, number)
    pair = lax.dynamic_slice_in_dim(table, 2 * chip, 2, 0)
    spot = lax.broadcasted_iota(jnp.int32, (devices // 2, 2 * capacity), 1) == picked[:, None]
    spot = spot & filled[:, None]
    slot_counts = masked_sum(spot, pair[:, 1 : 1 + capacity].reshape(1, -1), 1)
    slot_ids = masked_sum(spot, pair[:, 1 + capacity :].reshape(1, -1), 1)
    slot_ids = jnp.where(filled, slot_ids, -1)
    pooled = pooled_slots(heads, tails, slot_counts, weights)
    groups = READ_DEV * devices
    id_keys = lax.broadcasted_iota(jnp.int32, (groups, slot_ids.shape[0]), 0)
    members = (id_keys == slot_ids[None, :]).astype(jnp.float32)
    terms = jnp.dot(
        members, pooled, precision=lax.Precision.HIGHEST, preferred_element_type=jnp.float32
    )
    terms = terms.reshape(devices // 2, 2, READ_DEV, hidden)
    kept = lax.dynamic_index_in_dim(terms, core, 1, keepdims=False)
    sent = lax.dynamic_index_in_dim(terms, 1 - core, 1, keepdims=False).astype(jnp.bfloat16)
    both = kept + lax.ppermute(sent, "col_2", SWAP).astype(jnp.float32)
    rest = jnp.concatenate([tails, both.astype(jnp.bfloat16)], axis=1)
    rest, arrived = lax.optimization_barrier((rest, arrived))
    arrived_rest = lax.all_to_all(rest, CHIP, split_axis=0, concat_axis=0, tiled=True)

    order = lax.broadcasted_iota(jnp.int32, (G_DEV, 1), 0) * devices + me
    shape = (devices, devices)
    before = lax.broadcasted_iota(jnp.int32, shape, 1) <= lax.broadcasted_iota(jnp.int32, shape, 0)
    upto = masked_sum(before, live[None, :], 1)
    passed = upto[None, :] <= order
    source = jnp.sum(passed.astype(jnp.int32), axis=1)
    start = jnp.max(jnp.where(passed, upto[None, :], 0), axis=1)
    source_idx = order[:, 0] - start
    every = lax.broadcasted_iota(jnp.int32, (devices,), 0)
    hit = (every[None, :, None] == source[:, None, None]) & (
        lax.broadcasted_iota(jnp.int32, (1, 1, capacity), 2) == source_idx[:, None, None]
    )
    counts = jnp.sum(jnp.where(hit, table[None, :, 1 : 1 + capacity], 0), axis=(1, 2))
    chips = source >> 1
    node_out = placed_heads(arrived, chips, counts, weights, nodes)
    return tuple(finished(node_out, arrived_rest, chips, counts, weights))


def solution(mesh):
    split = Mesh(
        mesh.devices.reshape(mesh.shape["row"], 4, 4, 2), ("row", "col_0", "col_1", "col_2")
    )
    return jax.shard_map(
        body,
        mesh=split,
        in_specs=(
            P(ROW_COL, None, None),
            P(ROW_COL),
            P(ROW_COL, None, None),
            P(ROW_COL),
            P(ROW_COL),
            P(),
            P(),
            P(),
            P(),
            P(),
            P(),
            P(),
        ),
        out_specs=(P(ROW_COL, None, None), P(ROW_COL, None)),
        check_vma=False,
    )
```

```python
import functools

import jax
import jax.numpy as jnp
from jax import lax
from jax.experimental import pallas as pl
from jax.experimental.pallas import tpu as pltpu
from jax.sharding import Mesh
from jax.sharding import PartitionSpec as P

G_DEV = 32
READ_DEV = 8
ROW_COL = ("row", "col_0", "col_1", "col_2")
CHIP = ("row", "col_0", "col_1")
SWAP = [(0, 1), (1, 0)]
PACK_BITS = 3
PACK = 1 << PACK_BITS
POOL = 8
MLP_BITS = 3
HEAD_ROWS = 80
TAIL_BITS = 3
TAIL_GRAPHS = 1 << TAIL_BITS
MLP = 1 << MLP_BITS
VMEM_BYTES = 59 * 1024 * 1024
BLEND_BYTES = 56 * 1024 * 1024


def masked_sum(keep, values, axis):
    return jnp.sum(jnp.where(keep, values, 0), axis=axis)


def blend_kernel(
    first, where, scale, own, par, own_edges, par_edges, out, taken, made, taken_sem, made_sem
):
    core, offset, live_a, live_b = where[0], where[1], where[2], where[3]
    count, nodes, _ = taken.shape
    size = made.shape[1]
    wrap = 2 * count - 1
    node_index = lax.broadcasted_iota(jnp.int32, (nodes, own_edges.shape[-1]), 0)
    row_index = first + lax.broadcasted_iota(jnp.int32, (size, own_edges.shape[-1]), 0)

    def source_of(slot):
        number = (2 * slot + core - offset) & wrap
        filled = number < live_a + live_b
        from_b = number >= live_a
        index = jnp.where(filled, jnp.where(from_b, number - live_a, number), slot)
        return index, jnp.logical_xor(from_b, core == 1)

    @pl.loop(0, count)
    def _(slot):
        index, from_par = source_of(slot)
        sem = taken_sem.at[slot >> PACK_BITS]

        @pl.when(from_par)
        def _():
            pltpu.make_async_copy(par.at[index], taken.at[slot], sem).start()

        @pl.when(jnp.logical_not(from_par))
        def _():
            pltpu.make_async_copy(own.at[index], taken.at[slot], sem).start()

    def put(group):
        rows = pl.ds(group * PACK, PACK)
        return pltpu.make_async_copy(made.at[rows], out.at[rows], made_sem.at[group])

    @pl.loop(0, count // PACK)
    def _(group):
        pltpu.make_async_copy(
            own.at[pl.ds(0, PACK)], taken.at[pl.ds(group * PACK, PACK)], taken_sem.at[group]
        ).wait()
        slots = [group * PACK + lane for lane in range(PACK)]
        sources, targets = [], []
        for slot in slots:
            index, from_par = source_of(slot)
            edges = jnp.where(from_par, par_edges[index], own_edges[index])
            sources.append((node_index == edges[0:1, :]).astype(jnp.bfloat16))
            targets.append((row_index == edges[1:2, :]).astype(jnp.bfloat16))
        adjacency = [
            lax.dot_general(t, s, (((1,), (1,)), ((), ())), preferred_element_type=jnp.float32)
            for t, s in zip(targets, sources)
        ]
        features = [taken[slot] for slot in slots]
        neighbours = [
            jnp.dot(a.astype(jnp.bfloat16), f, preferred_element_type=jnp.float32)
            for a, f in zip(adjacency, features)
        ]
        for slot, f, n in zip(slots, features, neighbours):
            kept = f[first : first + size].astype(jnp.float32)
            made[slot] = (scale[0] * kept + n).astype(jnp.bfloat16)
        put(group).start()

    @pl.loop(0, count // PACK)
    def _(group):
        put(group).wait()


def blended_slots(own, par, own_edges, par_edges, where, scale, first, size):
    count, nodes, hidden = own.shape
    anywhere = pl.BlockSpec(memory_space=pl.ANY)
    vector = pl.BlockSpec(memory_space=pltpu.VMEM)
    scalar = pl.BlockSpec(memory_space=pltpu.SMEM)
    return pl.pallas_call(
        functools.partial(blend_kernel, first),
        out_shape=jax.ShapeDtypeStruct((count, size, hidden), jnp.bfloat16),
        in_specs=[scalar, scalar, anywhere, anywhere, vector, vector],
        out_specs=anywhere,
        scratch_shapes=[
            pltpu.VMEM((count, nodes, hidden), jnp.bfloat16),
            pltpu.VMEM((count, size, hidden), jnp.bfloat16),
            pltpu.SemaphoreType.DMA((count // PACK,)),
            pltpu.SemaphoreType.DMA((count // PACK,)),
        ],
        compiler_params=pltpu.CompilerParams(vmem_limit_bytes=BLEND_BYTES),
        cost_estimate=pl.CostEstimate(
            flops=2 * count * size * nodes * (own_edges.shape[-1] + hidden),
            bytes_accessed=4 * count * nodes * hidden,
            transcendentals=0,
        ),
        name="blend",
    )(where, scale, own, par, own_edges, par_edges)


def perceptron(rows, weights):
    w_first, b_first, w_second, b_second, w_third, b_third = weights
    for w, b in ((w_first, b_first), (w_second, b_second)):
        total = jnp.dot(rows, w[...], preferred_element_type=jnp.float32) + b[...]
        rows = jnp.maximum(total, 0.0).astype(jnp.bfloat16)
    return jnp.dot(rows, w_third[...], preferred_element_type=jnp.float32) + b_third[...]


def weight_specs(weights):
    return [pl.BlockSpec(w.shape, lambda i, *tables: (0, 0)) for w in weights]


def mlp_cost(rows, hidden):
    return pl.CostEstimate(
        flops=6 * rows * hidden * hidden, bytes_accessed=4 * rows * hidden, transcendentals=0
    )


def pool_kernel(counts, head_ref, tail_ref, *refs):
    weights, out = refs[:6], refs[6]
    step = pl.program_id(0)
    many, head, hidden = head_ref.shape
    tail = tail_ref.shape[1]
    rows = jnp.concatenate(
        [head_ref[...].reshape(many * head, hidden), tail_ref[...].reshape(many * tail, hidden)],
        axis=0,
    )
    result = perceptron(rows, weights)
    for lane in range(many):
        count = counts[step * many + lane]
        total = jnp.zeros((1, hidden), jnp.float32)
        for first, start, size in ((0, lane * head, head), (head, many * head + lane * tail, tail)):
            node_index = first + lax.broadcasted_iota(jnp.int32, (size, 1), 0)
            kept = jnp.where(node_index < count, result[start : start + size], 0.0)
            kept = kept.astype(jnp.bfloat16).astype(jnp.float32)
            total = total + jnp.sum(kept, axis=0, keepdims=True)
        out[lane : lane + 1, :] = total / jnp.maximum(count, 1).astype(jnp.float32)


def pooled_slots(heads, tails, counts, weights):
    count, head, hidden = heads.shape
    tail = tails.shape[1]
    return pl.pallas_call(
        pool_kernel,
        out_shape=jax.ShapeDtypeStruct((count, hidden), jnp.float32),
        grid_spec=pltpu.PrefetchScalarGridSpec(
            num_scalar_prefetch=1,
            grid=(count // POOL,),
            in_specs=[
                pl.BlockSpec((POOL, head, hidden), lambda i, *tables: (i, 0, 0)),
                pl.BlockSpec((POOL, tail, hidden), lambda i, *tables: (i, 0, 0)),
            ]
            + weight_specs(weights),
            out_specs=pl.BlockSpec((POOL, hidden), lambda i, *tables: (i, 0)),
        ),
        compiler_params=pltpu.CompilerParams(dimension_semantics=("arbitrary",)),
        cost_estimate=mlp_cost(count * (head + tail), hidden),
        name="pool",
    )(counts, heads, tails, *weights)


def place_kernel(chips, counts, arrived, *refs):
    weights, out, taken, made, taken_sem, made_sem = refs[:6], *refs[6:]
    count, nodes, hidden = taken.shape

    @pl.loop(0, count)
    def _(slot):
        pltpu.make_async_copy(
            arrived.at[chips[slot]], taken.at[slot], taken_sem.at[slot >> MLP_BITS]
        ).start()

    def put(group):
        rows = pl.ds(group * MLP, MLP)
        return pltpu.make_async_copy(
            made.at[rows], out.at[rows, pl.ds(0, nodes)], made_sem.at[group]
        )

    node_index = lax.broadcasted_iota(jnp.int32, (nodes, 1), 0)

    @pl.loop(0, count // MLP)
    def _(group):
        rows = pl.ds(group * MLP, MLP)
        pltpu.make_async_copy(
            arrived.at[pl.ds(0, MLP)], taken.at[rows], taken_sem.at[group]
        ).wait()
        result = perceptron(taken[rows].reshape(MLP * nodes, hidden), weights)
        for lane in range(MLP):
            slot = group * MLP + lane
            part = result[lane * nodes : (lane + 1) * nodes]
            made[slot] = jnp.where(node_index < counts[slot], part, 0.0).astype(jnp.bfloat16)
        put(group).start()

    @pl.loop(0, count // MLP)
    def _(group):
        put(group).wait()


def placed_heads(arrived, chips, counts, weights, nodes):
    _, head, hidden = arrived.shape
    anywhere = pl.BlockSpec(memory_space=pl.ANY)
    vector = pl.BlockSpec(memory_space=pltpu.VMEM)
    scalar = pl.BlockSpec(memory_space=pltpu.SMEM)
    return pl.pallas_call(
        place_kernel,
        out_shape=jax.ShapeDtypeStruct((G_DEV, nodes, hidden), jnp.bfloat16),
        in_specs=[scalar, scalar, anywhere] + [vector] * 6,
        out_specs=anywhere,
        scratch_shapes=[
            pltpu.VMEM((G_DEV, head, hidden), jnp.bfloat16),
            pltpu.VMEM((G_DEV, head, hidden), jnp.bfloat16),
            pltpu.SemaphoreType.DMA((G_DEV // MLP,)),
            pltpu.SemaphoreType.DMA((G_DEV // MLP,)),
        ],
        compiler_params=pltpu.CompilerParams(vmem_limit_bytes=VMEM_BYTES),
        cost_estimate=mlp_cost(G_DEV * head, hidden),
        name="place",
    )(chips, counts, arrived, *weights)


def finish_kernel(chips, counts, arrived, *refs):
    weights, refs = refs[:6], refs[7:]
    out, readout, taken, made, terms, taken_sem, made_sem, terms_sem = refs
    count, tail, hidden = taken.shape
    nodes = out.shape[1]
    own_rows = pl.ds(0, tail)

    @pl.loop(0, count)
    def _(slot):
        pltpu.make_async_copy(
            arrived.at[chips[slot], own_rows], taken.at[slot], taken_sem.at[slot >> TAIL_BITS]
        ).start()

    summed = pltpu.make_async_copy(arrived.at[:, pl.ds(tail, READ_DEV)], terms, terms_sem)
    summed.start()

    def put(group):
        rows = pl.ds(group * TAIL_GRAPHS, TAIL_GRAPHS)
        return pltpu.make_async_copy(
            made.at[rows], out.at[rows, pl.ds(nodes - tail, tail)], made_sem.at[group]
        )

    node_index = nodes - tail + lax.broadcasted_iota(jnp.int32, (tail, 1), 0)

    @pl.loop(0, count // TAIL_GRAPHS)
    def _(group):
        rows = pl.ds(group * TAIL_GRAPHS, TAIL_GRAPHS)
        pltpu.make_async_copy(
            arrived.at[pl.ds(0, TAIL_GRAPHS), own_rows], taken.at[rows], taken_sem.at[group]
        ).wait()
        result = perceptron(taken[rows].reshape(TAIL_GRAPHS * tail, hidden), weights)
        for lane in range(TAIL_GRAPHS):
            slot = group * TAIL_GRAPHS + lane
            part = result[lane * tail : (lane + 1) * tail]
            made[slot] = jnp.where(node_index < counts[slot], part, 0.0).astype(jnp.bfloat16)
        put(group).start()

    summed.wait()
    readout[...] = jnp.sum(terms[...].astype(jnp.float32), axis=0)

    @pl.loop(0, count // TAIL_GRAPHS)
    def _(group):
        put(group).wait()


def finished(node_out, arrived, chips, counts, weights):
    count, nodes, hidden = node_out.shape
    tail = arrived.shape[1] - READ_DEV
    anywhere = pl.BlockSpec(memory_space=pl.ANY)
    vector = pl.BlockSpec(memory_space=pltpu.VMEM)
    scalar = pl.BlockSpec(memory_space=pltpu.SMEM)
    return pl.pallas_call(
        finish_kernel,
        out_shape=[
            jax.ShapeDtypeStruct(node_out.shape, jnp.bfloat16),
            jax.ShapeDtypeStruct((READ_DEV, hidden), jnp.float32),
        ],
        in_specs=[scalar, scalar, anywhere] + [vector] * 6 + [anywhere],
        out_specs=[anywhere, vector],
        scratch_shapes=[
            pltpu.VMEM((count, tail, hidden), jnp.bfloat16),
            pltpu.VMEM((count, tail, hidden), jnp.bfloat16),
            pltpu.VMEM((arrived.shape[0], READ_DEV, hidden), jnp.bfloat16),
            pltpu.SemaphoreType.DMA((count // TAIL_GRAPHS,)),
            pltpu.SemaphoreType.DMA((count // TAIL_GRAPHS,)),
            pltpu.SemaphoreType.DMA,
        ],
        input_output_aliases={9: 0},
        compiler_params=pltpu.CompilerParams(vmem_limit_bytes=VMEM_BYTES),
        cost_estimate=mlp_cost(count * tail, hidden),
        name="finish",
    )(chips, counts, arrived, *weights, node_out)


def body(
    node_features,
    node_counts,
    edge_list,
    readout_ids,
    live_graphs,
    self_weight,
    w_first,
    b_first,
    w_second,
    b_second,
    w_third,
    b_third,
):
    weights = (
        w_first,
        b_first[None, :],
        w_second,
        b_second[None, :],
        w_third,
        b_third[None, :],
    )
    devices = lax.axis_size(ROW_COL)
    capacity, nodes, hidden = node_features.shape
    me = lax.axis_index(ROW_COL)
    core = lax.axis_index("col_2")
    chip = lax.axis_index(CHIP)

    par_features = lax.ppermute(node_features, "col_2", SWAP)
    par_edges = lax.ppermute(edge_list, "col_2", SWAP)
    info = jnp.concatenate([live_graphs, node_counts, readout_ids])
    table = lax.all_to_all(
        jnp.broadcast_to(info[None], (devices, info.shape[0])), ROW_COL, 0, 0, tiled=True
    )
    live = table[:, 0]

    device = lax.broadcasted_iota(jnp.int32, (4, devices), 1)
    part = lax.broadcasted_iota(jnp.int32, (4, devices), 0)
    ahead = (part == 1) & (device < 2 * chip)
    mine = (part >= 2) & (device == 2 * chip + part - 2)
    own = (part == 0) & (device < core)
    place = masked_sum(ahead | mine | own, jnp.where(own, 1, live[None, :]), 1)

    graphs = (node_features, par_features, edge_list, par_edges, place, self_weight)
    heads = blended_slots(*graphs, 0, HEAD_ROWS)
    arrived = lax.all_to_all(heads, CHIP, split_axis=0, concat_axis=0, tiled=True)
    tails = blended_slots(*graphs, HEAD_ROWS, nodes - HEAD_ROWS)

    offset, live_a, live_b = place[1], place[2], place[3]
    slot = lax.broadcasted_iota(jnp.int32, (devices // 2,), 0)
    number = (2 * slot + core - offset) & (devices - 1)
    filled = number < live_a + live_b
    picked = jnp.where(number >= live_a, capacity + number - live_a, number)
    pair = lax.dynamic_slice_in_dim(table, 2 * chip, 2, 0)
    spot = lax.broadcasted_iota(jnp.int32, (devices // 2, 2 * capacity), 1) == picked[:, None]
    spot = spot & filled[:, None]
    slot_counts = masked_sum(spot, pair[:, 1 : 1 + capacity].reshape(1, -1), 1)
    slot_ids = masked_sum(spot, pair[:, 1 + capacity :].reshape(1, -1), 1)
    slot_ids = jnp.where(filled, slot_ids, -1)
    pooled = pooled_slots(heads, tails, slot_counts, weights)
    groups = READ_DEV * devices
    id_keys = lax.broadcasted_iota(jnp.int32, (groups, slot_ids.shape[0]), 0)
    members = (id_keys == slot_ids[None, :]).astype(jnp.float32)
    terms = jnp.dot(
        members, pooled, precision=lax.Precision.HIGHEST, preferred_element_type=jnp.float32
    )
    terms = terms.reshape(devices // 2, 2, READ_DEV, hidden)
    kept = lax.dynamic_index_in_dim(terms, core, 1, keepdims=False)
    sent = lax.dynamic_index_in_dim(terms, 1 - core, 1, keepdims=False).astype(jnp.bfloat16)
    both = kept + lax.ppermute(sent, "col_2", SWAP).astype(jnp.float32)
    rest = jnp.concatenate([tails, both.astype(jnp.bfloat16)], axis=1)
    rest, arrived = lax.optimization_barrier((rest, arrived))
    arrived_rest = lax.all_to_all(rest, CHIP, split_axis=0, concat_axis=0, tiled=True)

    order = lax.broadcasted_iota(jnp.int32, (G_DEV, 1), 0) * devices + me
    shape = (devices, devices)
    before = lax.broadcasted_iota(jnp.int32, shape, 1) <= lax.broadcasted_iota(jnp.int32, shape, 0)
    upto = masked_sum(before, live[None, :], 1)
    passed = upto[None, :] <= order
    source = jnp.sum(passed.astype(jnp.int32), axis=1)
    start = jnp.max(jnp.where(passed, upto[None, :], 0), axis=1)
    source_idx = order[:, 0] - start
    every = lax.broadcasted_iota(jnp.int32, (devices,), 0)
    hit = (every[None, :, None] == source[:, None, None]) & (
        lax.broadcasted_iota(jnp.int32, (1, 1, capacity), 2) == source_idx[:, None, None]
    )
    counts = jnp.sum(jnp.where(hit, table[None, :, 1 : 1 + capacity], 0), axis=(1, 2))
    chips = source >> 1
    node_out = placed_heads(arrived, chips, counts, weights, nodes)
    return tuple(finished(node_out, arrived_rest, chips, counts, weights))


def solution(mesh):
    split = Mesh(
        mesh.devices.reshape(mesh.shape["row"], 4, 4, 2), ("row", "col_0", "col_1", "col_2")
    )
    return jax.shard_map(
        body,
        mesh=split,
        in_specs=(
            P(ROW_COL, None, None),
            P(ROW_COL),
            P(ROW_COL, None, None),
            P(ROW_COL),
            P(ROW_COL),
            P(),
            P(),
            P(),
            P(),
            P(),
            P(),
            P(),
        ),
        out_specs=(P(ROW_COL, None, None), P(ROW_COL, None)),
        check_vma=False,
    )
```

```python
import functools

import jax
import jax.numpy as jnp
from jax import lax
from jax.experimental import pallas as pl
from jax.experimental.pallas import tpu as pltpu
from jax.sharding import Mesh
from jax.sharding import PartitionSpec as P

G_DEV = 32
READ_DEV = 8
ROW_COL = ("row", "col_0", "col_1", "col_2")
CHIP = ("row", "col_0", "col_1")
SWAP = [(0, 1), (1, 0)]
PACK_BITS = 3
PACK = 1 << PACK_BITS
POOL = 8
MLP_BITS = 3
HEAD_ROWS = 80
TAIL_BITS = 5
TAIL_GRAPHS = 1 << TAIL_BITS
MLP = 1 << MLP_BITS
VMEM_BYTES = 59 * 1024 * 1024
BLEND_BYTES = 56 * 1024 * 1024


def masked_sum(keep, values, axis):
    return jnp.sum(jnp.where(keep, values, 0), axis=axis)


def blend_kernel(
    first, where, scale, own, par, own_edges, par_edges, out, taken, made, taken_sem, made_sem
):
    core, offset, live_a, live_b = where[0], where[1], where[2], where[3]
    count, nodes, _ = taken.shape
    size = made.shape[1]
    wrap = 2 * count - 1
    node_index = lax.broadcasted_iota(jnp.int32, (nodes, own_edges.shape[-1]), 0)
    row_index = first + lax.broadcasted_iota(jnp.int32, (size, own_edges.shape[-1]), 0)

    def source_of(slot):
        number = (2 * slot + core - offset) & wrap
        filled = number < live_a + live_b
        from_b = number >= live_a
        index = jnp.where(filled, jnp.where(from_b, number - live_a, number), slot)
        return index, jnp.logical_xor(from_b, core == 1)

    @pl.loop(0, count)
    def _(slot):
        index, from_par = source_of(slot)
        sem = taken_sem.at[slot >> PACK_BITS]

        @pl.when(from_par)
        def _():
            pltpu.make_async_copy(par.at[index], taken.at[slot], sem).start()

        @pl.when(jnp.logical_not(from_par))
        def _():
            pltpu.make_async_copy(own.at[index], taken.at[slot], sem).start()

    def put(group):
        rows = pl.ds(group * PACK, PACK)
        return pltpu.make_async_copy(made.at[rows], out.at[rows], made_sem.at[group])

    @pl.loop(0, count // PACK)
    def _(group):
        pltpu.make_async_copy(
            own.at[pl.ds(0, PACK)], taken.at[pl.ds(group * PACK, PACK)], taken_sem.at[group]
        ).wait()
        slots = [group * PACK + lane for lane in range(PACK)]
        sources, targets = [], []
        for slot in slots:
            index, from_par = source_of(slot)
            edges = jnp.where(from_par, par_edges[index], own_edges[index])
            sources.append((node_index == edges[0:1, :]).astype(jnp.bfloat16))
            targets.append((row_index == edges[1:2, :]).astype(jnp.bfloat16))
        adjacency = [
            lax.dot_general(t, s, (((1,), (1,)), ((), ())), preferred_element_type=jnp.float32)
            for t, s in zip(targets, sources)
        ]
        features = [taken[slot] for slot in slots]
        neighbours = [
            jnp.dot(a.astype(jnp.bfloat16), f, preferred_element_type=jnp.float32)
            for a, f in zip(adjacency, features)
        ]
        for slot, f, n in zip(slots, features, neighbours):
            kept = f[first : first + size].astype(jnp.float32)
            made[slot] = (scale[0] * kept + n).astype(jnp.bfloat16)
        put(group).start()

    @pl.loop(0, count // PACK)
    def _(group):
        put(group).wait()


def blended_slots(own, par, own_edges, par_edges, where, scale, first, size):
    count, nodes, hidden = own.shape
    anywhere = pl.BlockSpec(memory_space=pl.ANY)
    vector = pl.BlockSpec(memory_space=pltpu.VMEM)
    scalar = pl.BlockSpec(memory_space=pltpu.SMEM)
    return pl.pallas_call(
        functools.partial(blend_kernel, first),
        out_shape=jax.ShapeDtypeStruct((count, size, hidden), jnp.bfloat16),
        in_specs=[scalar, scalar, anywhere, anywhere, vector, vector],
        out_specs=anywhere,
        scratch_shapes=[
            pltpu.VMEM((count, nodes, hidden), jnp.bfloat16),
            pltpu.VMEM((count, size, hidden), jnp.bfloat16),
            pltpu.SemaphoreType.DMA((count // PACK,)),
            pltpu.SemaphoreType.DMA((count // PACK,)),
        ],
        compiler_params=pltpu.CompilerParams(vmem_limit_bytes=BLEND_BYTES),
        cost_estimate=pl.CostEstimate(
            flops=2 * count * size * nodes * (own_edges.shape[-1] + hidden),
            bytes_accessed=4 * count * nodes * hidden,
            transcendentals=0,
        ),
        name="blend",
    )(where, scale, own, par, own_edges, par_edges)


def perceptron(rows, weights):
    w_first, b_first, w_second, b_second, w_third, b_third = weights
    for w, b in ((w_first, b_first), (w_second, b_second)):
        total = jnp.dot(rows, w[...], preferred_element_type=jnp.float32) + b[...]
        rows = jnp.maximum(total, 0.0).astype(jnp.bfloat16)
    return jnp.dot(rows, w_third[...], preferred_element_type=jnp.float32) + b_third[...]


def weight_specs(weights):
    return [pl.BlockSpec(w.shape, lambda i, *tables: (0, 0)) for w in weights]


def mlp_cost(rows, hidden):
    return pl.CostEstimate(
        flops=6 * rows * hidden * hidden, bytes_accessed=4 * rows * hidden, transcendentals=0
    )


def pool_kernel(counts, head_ref, tail_ref, *refs):
    weights, out = refs[:6], refs[6]
    step = pl.program_id(0)
    many, head, hidden = head_ref.shape
    tail = tail_ref.shape[1]
    rows = jnp.concatenate(
        [head_ref[...].reshape(many * head, hidden), tail_ref[...].reshape(many * tail, hidden)],
        axis=0,
    )
    result = perceptron(rows, weights)
    for lane in range(many):
        count = counts[step * many + lane]
        total = jnp.zeros((1, hidden), jnp.float32)
        for first, start, size in ((0, lane * head, head), (head, many * head + lane * tail, tail)):
            node_index = first + lax.broadcasted_iota(jnp.int32, (size, 1), 0)
            kept = jnp.where(node_index < count, result[start : start + size], 0.0)
            kept = kept.astype(jnp.bfloat16).astype(jnp.float32)
            total = total + jnp.sum(kept, axis=0, keepdims=True)
        out[lane : lane + 1, :] = total / jnp.maximum(count, 1).astype(jnp.float32)


def pooled_slots(heads, tails, counts, weights):
    count, head, hidden = heads.shape
    tail = tails.shape[1]
    return pl.pallas_call(
        pool_kernel,
        out_shape=jax.ShapeDtypeStruct((count, hidden), jnp.float32),
        grid_spec=pltpu.PrefetchScalarGridSpec(
            num_scalar_prefetch=1,
            grid=(count // POOL,),
            in_specs=[
                pl.BlockSpec((POOL, head, hidden), lambda i, *tables: (i, 0, 0)),
                pl.BlockSpec((POOL, tail, hidden), lambda i, *tables: (i, 0, 0)),
            ]
            + weight_specs(weights),
            out_specs=pl.BlockSpec((POOL, hidden), lambda i, *tables: (i, 0)),
        ),
        compiler_params=pltpu.CompilerParams(dimension_semantics=("arbitrary",)),
        cost_estimate=mlp_cost(count * (head + tail), hidden),
        name="pool",
    )(counts, heads, tails, *weights)


def place_kernel(chips, counts, arrived, *refs):
    weights, out, taken, made, taken_sem, made_sem = refs[:6], *refs[6:]
    count, nodes, hidden = taken.shape

    @pl.loop(0, count)
    def _(slot):
        pltpu.make_async_copy(
            arrived.at[chips[slot]], taken.at[slot], taken_sem.at[slot >> MLP_BITS]
        ).start()

    def put(group):
        rows = pl.ds(group * MLP, MLP)
        return pltpu.make_async_copy(
            made.at[rows], out.at[rows, pl.ds(0, nodes)], made_sem.at[group]
        )

    node_index = lax.broadcasted_iota(jnp.int32, (nodes, 1), 0)

    @pl.loop(0, count // MLP)
    def _(group):
        rows = pl.ds(group * MLP, MLP)
        pltpu.make_async_copy(
            arrived.at[pl.ds(0, MLP)], taken.at[rows], taken_sem.at[group]
        ).wait()
        result = perceptron(taken[rows].reshape(MLP * nodes, hidden), weights)
        for lane in range(MLP):
            slot = group * MLP + lane
            part = result[lane * nodes : (lane + 1) * nodes]
            made[slot] = jnp.where(node_index < counts[slot], part, 0.0).astype(jnp.bfloat16)
        put(group).start()

    @pl.loop(0, count // MLP)
    def _(group):
        put(group).wait()


def placed_heads(arrived, chips, counts, weights, nodes):
    _, head, hidden = arrived.shape
    anywhere = pl.BlockSpec(memory_space=pl.ANY)
    vector = pl.BlockSpec(memory_space=pltpu.VMEM)
    scalar = pl.BlockSpec(memory_space=pltpu.SMEM)
    return pl.pallas_call(
        place_kernel,
        out_shape=jax.ShapeDtypeStruct((G_DEV, nodes, hidden), jnp.bfloat16),
        in_specs=[scalar, scalar, anywhere] + [vector] * 6,
        out_specs=anywhere,
        scratch_shapes=[
            pltpu.VMEM((G_DEV, head, hidden), jnp.bfloat16),
            pltpu.VMEM((G_DEV, head, hidden), jnp.bfloat16),
            pltpu.SemaphoreType.DMA((G_DEV // MLP,)),
            pltpu.SemaphoreType.DMA((G_DEV // MLP,)),
        ],
        compiler_params=pltpu.CompilerParams(vmem_limit_bytes=VMEM_BYTES),
        cost_estimate=mlp_cost(G_DEV * head, hidden),
        name="place",
    )(chips, counts, arrived, *weights)


def finish_kernel(chips, counts, arrived, *refs):
    weights, refs = refs[:6], refs[7:]
    out, readout, taken, made, terms, taken_sem, made_sem, terms_sem = refs
    count, tail, hidden = taken.shape
    nodes = out.shape[1]
    own_rows = pl.ds(0, tail)

    @pl.loop(0, count)
    def _(slot):
        pltpu.make_async_copy(
            arrived.at[chips[slot], own_rows], taken.at[slot], taken_sem.at[slot >> TAIL_BITS]
        ).start()

    summed = pltpu.make_async_copy(arrived.at[:, pl.ds(tail, READ_DEV)], terms, terms_sem)
    summed.start()

    def put(group):
        rows = pl.ds(group * TAIL_GRAPHS, TAIL_GRAPHS)
        return pltpu.make_async_copy(
            made.at[rows], out.at[rows, pl.ds(nodes - tail, tail)], made_sem.at[group]
        )

    node_index = nodes - tail + lax.broadcasted_iota(jnp.int32, (tail, 1), 0)

    @pl.loop(0, count // TAIL_GRAPHS)
    def _(group):
        rows = pl.ds(group * TAIL_GRAPHS, TAIL_GRAPHS)
        pltpu.make_async_copy(
            arrived.at[pl.ds(0, TAIL_GRAPHS), own_rows], taken.at[rows], taken_sem.at[group]
        ).wait()
        result = perceptron(taken[rows].reshape(TAIL_GRAPHS * tail, hidden), weights)
        for lane in range(TAIL_GRAPHS):
            slot = group * TAIL_GRAPHS + lane
            part = result[lane * tail : (lane + 1) * tail]
            made[slot] = jnp.where(node_index < counts[slot], part, 0.0).astype(jnp.bfloat16)
        put(group).start()

    summed.wait()
    readout[...] = jnp.sum(terms[...].astype(jnp.float32), axis=0)

    @pl.loop(0, count // TAIL_GRAPHS)
    def _(group):
        put(group).wait()


def finished(node_out, arrived, chips, counts, weights):
    count, nodes, hidden = node_out.shape
    tail = arrived.shape[1] - READ_DEV
    anywhere = pl.BlockSpec(memory_space=pl.ANY)
    vector = pl.BlockSpec(memory_space=pltpu.VMEM)
    scalar = pl.BlockSpec(memory_space=pltpu.SMEM)
    return pl.pallas_call(
        finish_kernel,
        out_shape=[
            jax.ShapeDtypeStruct(node_out.shape, jnp.bfloat16),
            jax.ShapeDtypeStruct((READ_DEV, hidden), jnp.float32),
        ],
        in_specs=[scalar, scalar, anywhere] + [vector] * 6 + [anywhere],
        out_specs=[anywhere, vector],
        scratch_shapes=[
            pltpu.VMEM((count, tail, hidden), jnp.bfloat16),
            pltpu.VMEM((count, tail, hidden), jnp.bfloat16),
            pltpu.VMEM((arrived.shape[0], READ_DEV, hidden), jnp.bfloat16),
            pltpu.SemaphoreType.DMA((count // TAIL_GRAPHS,)),
            pltpu.SemaphoreType.DMA((count // TAIL_GRAPHS,)),
            pltpu.SemaphoreType.DMA,
        ],
        input_output_aliases={9: 0},
        compiler_params=pltpu.CompilerParams(vmem_limit_bytes=VMEM_BYTES),
        cost_estimate=mlp_cost(count * tail, hidden),
        name="finish",
    )(chips, counts, arrived, *weights, node_out)


def body(
    node_features,
    node_counts,
    edge_list,
    readout_ids,
    live_graphs,
    self_weight,
    w_first,
    b_first,
    w_second,
    b_second,
    w_third,
    b_third,
):
    weights = (
        w_first,
        b_first[None, :],
        w_second,
        b_second[None, :],
        w_third,
        b_third[None, :],
    )
    devices = lax.axis_size(ROW_COL)
    capacity, nodes, hidden = node_features.shape
    me = lax.axis_index(ROW_COL)
    core = lax.axis_index("col_2")
    chip = lax.axis_index(CHIP)

    par_features = lax.ppermute(node_features, "col_2", SWAP)
    par_edges = lax.ppermute(edge_list, "col_2", SWAP)
    info = jnp.concatenate([live_graphs, node_counts, readout_ids])
    table = lax.all_to_all(
        jnp.broadcast_to(info[None], (devices, info.shape[0])), ROW_COL, 0, 0, tiled=True
    )
    live = table[:, 0]

    device = lax.broadcasted_iota(jnp.int32, (4, devices), 1)
    part = lax.broadcasted_iota(jnp.int32, (4, devices), 0)
    ahead = (part == 1) & (device < 2 * chip)
    mine = (part >= 2) & (device == 2 * chip + part - 2)
    own = (part == 0) & (device < core)
    place = masked_sum(ahead | mine | own, jnp.where(own, 1, live[None, :]), 1)

    graphs = (node_features, par_features, edge_list, par_edges, place, self_weight)
    heads = blended_slots(*graphs, 0, HEAD_ROWS)
    arrived = lax.all_to_all(heads, CHIP, split_axis=0, concat_axis=0, tiled=True)
    tails = blended_slots(*graphs, HEAD_ROWS, nodes - HEAD_ROWS)

    offset, live_a, live_b = place[1], place[2], place[3]
    slot = lax.broadcasted_iota(jnp.int32, (devices // 2,), 0)
    number = (2 * slot + core - offset) & (devices - 1)
    filled = number < live_a + live_b
    picked = jnp.where(number >= live_a, capacity + number - live_a, number)
    pair = lax.dynamic_slice_in_dim(table, 2 * chip, 2, 0)
    spot = lax.broadcasted_iota(jnp.int32, (devices // 2, 2 * capacity), 1) == picked[:, None]
    spot = spot & filled[:, None]
    slot_counts = masked_sum(spot, pair[:, 1 : 1 + capacity].reshape(1, -1), 1)
    slot_ids = masked_sum(spot, pair[:, 1 + capacity :].reshape(1, -1), 1)
    slot_ids = jnp.where(filled, slot_ids, -1)
    pooled = pooled_slots(heads, tails, slot_counts, weights)
    groups = READ_DEV * devices
    id_keys = lax.broadcasted_iota(jnp.int32, (groups, slot_ids.shape[0]), 0)
    members = (id_keys == slot_ids[None, :]).astype(jnp.float32)
    terms = jnp.dot(
        members, pooled, precision=lax.Precision.HIGHEST, preferred_element_type=jnp.float32
    )
    terms = terms.reshape(devices // 2, 2, READ_DEV, hidden)
    kept = lax.dynamic_index_in_dim(terms, core, 1, keepdims=False)
    sent = lax.dynamic_index_in_dim(terms, 1 - core, 1, keepdims=False).astype(jnp.bfloat16)
    both = kept + lax.ppermute(sent, "col_2", SWAP).astype(jnp.float32)
    rest = jnp.concatenate([tails, both.astype(jnp.bfloat16)], axis=1)
    rest, arrived = lax.optimization_barrier((rest, arrived))
    arrived_rest = lax.all_to_all(rest, CHIP, split_axis=0, concat_axis=0, tiled=True)

    order = lax.broadcasted_iota(jnp.int32, (G_DEV, 1), 0) * devices + me
    shape = (devices, devices)
    before = lax.broadcasted_iota(jnp.int32, shape, 1) <= lax.broadcasted_iota(jnp.int32, shape, 0)
    upto = masked_sum(before, live[None, :], 1)
    passed = upto[None, :] <= order
    source = jnp.sum(passed.astype(jnp.int32), axis=1)
    start = jnp.max(jnp.where(passed, upto[None, :], 0), axis=1)
    source_idx = order[:, 0] - start
    every = lax.broadcasted_iota(jnp.int32, (devices,), 0)
    hit = (every[None, :, None] == source[:, None, None]) & (
        lax.broadcasted_iota(jnp.int32, (1, 1, capacity), 2) == source_idx[:, None, None]
    )
    counts = jnp.sum(jnp.where(hit, table[None, :, 1 : 1 + capacity], 0), axis=(1, 2))
    chips = source >> 1
    node_out = placed_heads(arrived, chips, counts, weights, nodes)
    return tuple(finished(node_out, arrived_rest, chips, counts, weights))


def solution(mesh):
    split = Mesh(
        mesh.devices.reshape(mesh.shape["row"], 4, 4, 2), ("row", "col_0", "col_1", "col_2")
    )
    return jax.shard_map(
        body,
        mesh=split,
        in_specs=(
            P(ROW_COL, None, None),
            P(ROW_COL),
            P(ROW_COL, None, None),
            P(ROW_COL),
            P(ROW_COL),
            P(),
            P(),
            P(),
            P(),
            P(),
            P(),
            P(),
        ),
        out_specs=(P(ROW_COL, None, None), P(ROW_COL, None)),
        check_vma=False,
    )
```

```python
import functools

import jax
import jax.numpy as jnp
from jax import lax
from jax.experimental import pallas as pl
from jax.experimental.pallas import tpu as pltpu
from jax.sharding import Mesh
from jax.sharding import PartitionSpec as P

G_DEV = 32
READ_DEV = 8
ROW_COL = ("row", "col_0", "col_1", "col_2")
CHIP = ("row", "col_0", "col_1")
SWAP = [(0, 1), (1, 0)]
PACK_BITS = 3
PACK = 1 << PACK_BITS
POOL = 8
MLP_BITS = 3
HEAD_ROWS = 80
TAIL_BITS = 4
TAIL_GRAPHS = 1 << TAIL_BITS
MLP = 1 << MLP_BITS
VMEM_BYTES = 59 * 1024 * 1024
FINISH_BYTES = 40 * 1024 * 1024
BLEND_BYTES = 56 * 1024 * 1024


def masked_sum(keep, values, axis):
    return jnp.sum(jnp.where(keep, values, 0), axis=axis)


def blend_kernel(
    first, where, scale, own, par, own_edges, par_edges, out, taken, made, taken_sem, made_sem
):
    core, offset, live_a, live_b = where[0], where[1], where[2], where[3]
    count, nodes, _ = taken.shape
    size = made.shape[1]
    wrap = 2 * count - 1
    node_index = lax.broadcasted_iota(jnp.int32, (nodes, own_edges.shape[-1]), 0)
    row_index = first + lax.broadcasted_iota(jnp.int32, (size, own_edges.shape[-1]), 0)

    def source_of(slot):
        number = (2 * slot + core - offset) & wrap
        filled = number < live_a + live_b
        from_b = number >= live_a
        index = jnp.where(filled, jnp.where(from_b, number - live_a, number), slot)
        return index, jnp.logical_xor(from_b, core == 1)

    @pl.loop(0, count)
    def _(slot):
        index, from_par = source_of(slot)
        sem = taken_sem.at[slot >> PACK_BITS]

        @pl.when(from_par)
        def _():
            pltpu.make_async_copy(par.at[index], taken.at[slot], sem).start()

        @pl.when(jnp.logical_not(from_par))
        def _():
            pltpu.make_async_copy(own.at[index], taken.at[slot], sem).start()

    def put(group):
        rows = pl.ds(group * PACK, PACK)
        return pltpu.make_async_copy(made.at[rows], out.at[rows], made_sem.at[group])

    @pl.loop(0, count // PACK)
    def _(group):
        pltpu.make_async_copy(
            own.at[pl.ds(0, PACK)], taken.at[pl.ds(group * PACK, PACK)], taken_sem.at[group]
        ).wait()
        slots = [group * PACK + lane for lane in range(PACK)]
        sources, targets = [], []
        for slot in slots:
            index, from_par = source_of(slot)
            edges = jnp.where(from_par, par_edges[index], own_edges[index])
            sources.append((node_index == edges[0:1, :]).astype(jnp.bfloat16))
            targets.append((row_index == edges[1:2, :]).astype(jnp.bfloat16))
        adjacency = [
            lax.dot_general(t, s, (((1,), (1,)), ((), ())), preferred_element_type=jnp.float32)
            for t, s in zip(targets, sources)
        ]
        features = [taken[slot] for slot in slots]
        neighbours = [
            jnp.dot(a.astype(jnp.bfloat16), f, preferred_element_type=jnp.float32)
            for a, f in zip(adjacency, features)
        ]
        for slot, f, n in zip(slots, features, neighbours):
            kept = f[first : first + size].astype(jnp.float32)
            made[slot] = (scale[0] * kept + n).astype(jnp.bfloat16)
        put(group).start()

    @pl.loop(0, count // PACK)
    def _(group):
        put(group).wait()


def blended_slots(own, par, own_edges, par_edges, where, scale, first, size):
    count, nodes, hidden = own.shape
    anywhere = pl.BlockSpec(memory_space=pl.ANY)
    vector = pl.BlockSpec(memory_space=pltpu.VMEM)
    scalar = pl.BlockSpec(memory_space=pltpu.SMEM)
    return pl.pallas_call(
        functools.partial(blend_kernel, first),
        out_shape=jax.ShapeDtypeStruct((count, size, hidden), jnp.bfloat16),
        in_specs=[scalar, scalar, anywhere, anywhere, vector, vector],
        out_specs=anywhere,
        scratch_shapes=[
            pltpu.VMEM((count, nodes, hidden), jnp.bfloat16),
            pltpu.VMEM((count, size, hidden), jnp.bfloat16),
            pltpu.SemaphoreType.DMA((count // PACK,)),
            pltpu.SemaphoreType.DMA((count // PACK,)),
        ],
        compiler_params=pltpu.CompilerParams(vmem_limit_bytes=BLEND_BYTES),
        cost_estimate=pl.CostEstimate(
            flops=2 * count * size * nodes * (own_edges.shape[-1] + hidden),
            bytes_accessed=4 * count * nodes * hidden,
            transcendentals=0,
        ),
        name="blend",
    )(where, scale, own, par, own_edges, par_edges)


def perceptron(rows, weights):
    w_first, b_first, w_second, b_second, w_third, b_third = weights
    for w, b in ((w_first, b_first), (w_second, b_second)):
        total = jnp.dot(rows, w[...], preferred_element_type=jnp.float32) + b[...]
        rows = jnp.maximum(total, 0.0).astype(jnp.bfloat16)
    return jnp.dot(rows, w_third[...], preferred_element_type=jnp.float32) + b_third[...]


def weight_specs(weights):
    return [pl.BlockSpec(w.shape, lambda i, *tables: (0, 0)) for w in weights]


def mlp_cost(rows, hidden):
    return pl.CostEstimate(
        flops=6 * rows * hidden * hidden, bytes_accessed=4 * rows * hidden, transcendentals=0
    )


def pool_kernel(counts, head_ref, tail_ref, *refs):
    weights, out = refs[:6], refs[6]
    step = pl.program_id(0)
    many, head, hidden = head_ref.shape
    tail = tail_ref.shape[1]
    rows = jnp.concatenate(
        [head_ref[...].reshape(many * head, hidden), tail_ref[...].reshape(many * tail, hidden)],
        axis=0,
    )
    result = perceptron(rows, weights)
    for lane in range(many):
        count = counts[step * many + lane]
        total = jnp.zeros((1, hidden), jnp.float32)
        for first, start, size in ((0, lane * head, head), (head, many * head + lane * tail, tail)):
            node_index = first + lax.broadcasted_iota(jnp.int32, (size, 1), 0)
            kept = jnp.where(node_index < count, result[start : start + size], 0.0)
            kept = kept.astype(jnp.bfloat16).astype(jnp.float32)
            total = total + jnp.sum(kept, axis=0, keepdims=True)
        out[lane : lane + 1, :] = total / jnp.maximum(count, 1).astype(jnp.float32)


def pooled_slots(heads, tails, counts, weights):
    count, head, hidden = heads.shape
    tail = tails.shape[1]
    return pl.pallas_call(
        pool_kernel,
        out_shape=jax.ShapeDtypeStruct((count, hidden), jnp.float32),
        grid_spec=pltpu.PrefetchScalarGridSpec(
            num_scalar_prefetch=1,
            grid=(count // POOL,),
            in_specs=[
                pl.BlockSpec((POOL, head, hidden), lambda i, *tables: (i, 0, 0)),
                pl.BlockSpec((POOL, tail, hidden), lambda i, *tables: (i, 0, 0)),
            ]
            + weight_specs(weights),
            out_specs=pl.BlockSpec((POOL, hidden), lambda i, *tables: (i, 0)),
        ),
        compiler_params=pltpu.CompilerParams(dimension_semantics=("arbitrary",)),
        cost_estimate=mlp_cost(count * (head + tail), hidden),
        name="pool",
    )(counts, heads, tails, *weights)


def place_kernel(chips, counts, arrived, *refs):
    weights, out, taken, made, taken_sem, made_sem = refs[:6], *refs[6:]
    count, nodes, hidden = taken.shape

    @pl.loop(0, count)
    def _(slot):
        pltpu.make_async_copy(
            arrived.at[chips[slot]], taken.at[slot], taken_sem.at[slot >> MLP_BITS]
        ).start()

    def put(group):
        rows = pl.ds(group * MLP, MLP)
        return pltpu.make_async_copy(
            made.at[rows], out.at[rows, pl.ds(0, nodes)], made_sem.at[group]
        )

    node_index = lax.broadcasted_iota(jnp.int32, (nodes, 1), 0)

    @pl.loop(0, count // MLP)
    def _(group):
        rows = pl.ds(group * MLP, MLP)
        pltpu.make_async_copy(
            arrived.at[pl.ds(0, MLP)], taken.at[rows], taken_sem.at[group]
        ).wait()
        result = perceptron(taken[rows].reshape(MLP * nodes, hidden), weights)
        for lane in range(MLP):
            slot = group * MLP + lane
            part = result[lane * nodes : (lane + 1) * nodes]
            made[slot] = jnp.where(node_index < counts[slot], part, 0.0).astype(jnp.bfloat16)
        put(group).start()

    @pl.loop(0, count // MLP)
    def _(group):
        put(group).wait()


def placed_heads(arrived, chips, counts, weights, nodes):
    _, head, hidden = arrived.shape
    anywhere = pl.BlockSpec(memory_space=pl.ANY)
    vector = pl.BlockSpec(memory_space=pltpu.VMEM)
    scalar = pl.BlockSpec(memory_space=pltpu.SMEM)
    return pl.pallas_call(
        place_kernel,
        out_shape=jax.ShapeDtypeStruct((G_DEV, nodes, hidden), jnp.bfloat16),
        in_specs=[scalar, scalar, anywhere] + [vector] * 6,
        out_specs=anywhere,
        scratch_shapes=[
            pltpu.VMEM((G_DEV, head, hidden), jnp.bfloat16),
            pltpu.VMEM((G_DEV, head, hidden), jnp.bfloat16),
            pltpu.SemaphoreType.DMA((G_DEV // MLP,)),
            pltpu.SemaphoreType.DMA((G_DEV // MLP,)),
        ],
        compiler_params=pltpu.CompilerParams(vmem_limit_bytes=VMEM_BYTES),
        cost_estimate=mlp_cost(G_DEV * head, hidden),
        name="place",
    )(chips, counts, arrived, *weights)


def finish_kernel(chips, counts, arrived, *refs):
    weights, refs = refs[:6], refs[7:]
    out, readout, taken, made, terms, taken_sem, made_sem, terms_sem = refs
    count, tail, hidden = taken.shape
    nodes = out.shape[1]
    own_rows = pl.ds(0, tail)

    @pl.loop(0, count)
    def _(slot):
        pltpu.make_async_copy(
            arrived.at[chips[slot], own_rows], taken.at[slot], taken_sem.at[slot >> TAIL_BITS]
        ).start()

    summed = pltpu.make_async_copy(arrived.at[:, pl.ds(tail, READ_DEV)], terms, terms_sem)
    summed.start()

    def put(group):
        rows = pl.ds(group * TAIL_GRAPHS, TAIL_GRAPHS)
        return pltpu.make_async_copy(
            made.at[rows], out.at[rows, pl.ds(nodes - tail, tail)], made_sem.at[group]
        )

    node_index = nodes - tail + lax.broadcasted_iota(jnp.int32, (tail, 1), 0)

    @pl.loop(0, count // TAIL_GRAPHS)
    def _(group):
        rows = pl.ds(group * TAIL_GRAPHS, TAIL_GRAPHS)
        pltpu.make_async_copy(
            arrived.at[pl.ds(0, TAIL_GRAPHS), own_rows], taken.at[rows], taken_sem.at[group]
        ).wait()
        result = perceptron(taken[rows].reshape(TAIL_GRAPHS * tail, hidden), weights)
        for lane in range(TAIL_GRAPHS):
            slot = group * TAIL_GRAPHS + lane
            part = result[lane * tail : (lane + 1) * tail]
            made[slot] = jnp.where(node_index < counts[slot], part, 0.0).astype(jnp.bfloat16)
        put(group).start()

    summed.wait()
    readout[...] = jnp.sum(terms[...].astype(jnp.float32), axis=0)

    @pl.loop(0, count // TAIL_GRAPHS)
    def _(group):
        put(group).wait()


def finished(node_out, arrived, chips, counts, weights):
    count, nodes, hidden = node_out.shape
    tail = arrived.shape[1] - READ_DEV
    anywhere = pl.BlockSpec(memory_space=pl.ANY)
    vector = pl.BlockSpec(memory_space=pltpu.VMEM)
    scalar = pl.BlockSpec(memory_space=pltpu.SMEM)
    return pl.pallas_call(
        finish_kernel,
        out_shape=[
            jax.ShapeDtypeStruct(node_out.shape, jnp.bfloat16),
            jax.ShapeDtypeStruct((READ_DEV, hidden), jnp.float32),
        ],
        in_specs=[scalar, scalar, anywhere] + [vector] * 6 + [anywhere],
        out_specs=[anywhere, vector],
        scratch_shapes=[
            pltpu.VMEM((count, tail, hidden), jnp.bfloat16),
            pltpu.VMEM((count, tail, hidden), jnp.bfloat16),
            pltpu.VMEM((arrived.shape[0], READ_DEV, hidden), jnp.bfloat16),
            pltpu.SemaphoreType.DMA((count // TAIL_GRAPHS,)),
            pltpu.SemaphoreType.DMA((count // TAIL_GRAPHS,)),
            pltpu.SemaphoreType.DMA,
        ],
        input_output_aliases={9: 0},
        compiler_params=pltpu.CompilerParams(vmem_limit_bytes=FINISH_BYTES),
        cost_estimate=mlp_cost(count * tail, hidden),
        name="finish",
    )(chips, counts, arrived, *weights, node_out)


def body(
    node_features,
    node_counts,
    edge_list,
    readout_ids,
    live_graphs,
    self_weight,
    w_first,
    b_first,
    w_second,
    b_second,
    w_third,
    b_third,
):
    weights = (
        w_first,
        b_first[None, :],
        w_second,
        b_second[None, :],
        w_third,
        b_third[None, :],
    )
    devices = lax.axis_size(ROW_COL)
    capacity, nodes, hidden = node_features.shape
    me = lax.axis_index(ROW_COL)
    core = lax.axis_index("col_2")
    chip = lax.axis_index(CHIP)

    par_features = lax.ppermute(node_features, "col_2", SWAP)
    par_edges = lax.ppermute(edge_list, "col_2", SWAP)
    info = jnp.concatenate([live_graphs, node_counts, readout_ids])
    table = lax.all_to_all(
        jnp.broadcast_to(info[None], (devices, info.shape[0])), ROW_COL, 0, 0, tiled=True
    )
    live = table[:, 0]

    device = lax.broadcasted_iota(jnp.int32, (4, devices), 1)
    part = lax.broadcasted_iota(jnp.int32, (4, devices), 0)
    ahead = (part == 1) & (device < 2 * chip)
    mine = (part >= 2) & (device == 2 * chip + part - 2)
    own = (part == 0) & (device < core)
    place = masked_sum(ahead | mine | own, jnp.where(own, 1, live[None, :]), 1)

    graphs = (node_features, par_features, edge_list, par_edges, place, self_weight)
    heads = blended_slots(*graphs, 0, HEAD_ROWS)
    arrived = lax.all_to_all(heads, CHIP, split_axis=0, concat_axis=0, tiled=True)
    tails = blended_slots(*graphs, HEAD_ROWS, nodes - HEAD_ROWS)

    offset, live_a, live_b = place[1], place[2], place[3]
    slot = lax.broadcasted_iota(jnp.int32, (devices // 2,), 0)
    number = (2 * slot + core - offset) & (devices - 1)
    filled = number < live_a + live_b
    picked = jnp.where(number >= live_a, capacity + number - live_a, number)
    pair = lax.dynamic_slice_in_dim(table, 2 * chip, 2, 0)
    spot = lax.broadcasted_iota(jnp.int32, (devices // 2, 2 * capacity), 1) == picked[:, None]
    spot = spot & filled[:, None]
    slot_counts = masked_sum(spot, pair[:, 1 : 1 + capacity].reshape(1, -1), 1)
    slot_ids = masked_sum(spot, pair[:, 1 + capacity :].reshape(1, -1), 1)
    slot_ids = jnp.where(filled, slot_ids, -1)
    pooled = pooled_slots(heads, tails, slot_counts, weights)
    groups = READ_DEV * devices
    id_keys = lax.broadcasted_iota(jnp.int32, (groups, slot_ids.shape[0]), 0)
    members = (id_keys == slot_ids[None, :]).astype(jnp.float32)
    terms = jnp.dot(
        members, pooled, precision=lax.Precision.HIGHEST, preferred_element_type=jnp.float32
    )
    terms = terms.reshape(devices // 2, 2, READ_DEV, hidden)
    kept = lax.dynamic_index_in_dim(terms, core, 1, keepdims=False)
    sent = lax.dynamic_index_in_dim(terms, 1 - core, 1, keepdims=False).astype(jnp.bfloat16)
    both = kept + lax.ppermute(sent, "col_2", SWAP).astype(jnp.float32)
    rest = jnp.concatenate([tails, both.astype(jnp.bfloat16)], axis=1)
    rest, arrived = lax.optimization_barrier((rest, arrived))
    arrived_rest = lax.all_to_all(rest, CHIP, split_axis=0, concat_axis=0, tiled=True)

    order = lax.broadcasted_iota(jnp.int32, (G_DEV, 1), 0) * devices + me
    shape = (devices, devices)
    before = lax.broadcasted_iota(jnp.int32, shape, 1) <= lax.broadcasted_iota(jnp.int32, shape, 0)
    upto = masked_sum(before, live[None, :], 1)
    passed = upto[None, :] <= order
    source = jnp.sum(passed.astype(jnp.int32), axis=1)
    start = jnp.max(jnp.where(passed, upto[None, :], 0), axis=1)
    source_idx = order[:, 0] - start
    every = lax.broadcasted_iota(jnp.int32, (devices,), 0)
    hit = (every[None, :, None] == source[:, None, None]) & (
        lax.broadcasted_iota(jnp.int32, (1, 1, capacity), 2) == source_idx[:, None, None]
    )
    counts = jnp.sum(jnp.where(hit, table[None, :, 1 : 1 + capacity], 0), axis=(1, 2))
    chips = source >> 1
    node_out = placed_heads(arrived, chips, counts, weights, nodes)
    return tuple(finished(node_out, arrived_rest, chips, counts, weights))


def solution(mesh):
    split = Mesh(
        mesh.devices.reshape(mesh.shape["row"], 4, 4, 2), ("row", "col_0", "col_1", "col_2")
    )
    return jax.shard_map(
        body,
        mesh=split,
        in_specs=(
            P(ROW_COL, None, None),
            P(ROW_COL),
            P(ROW_COL, None, None),
            P(ROW_COL),
            P(ROW_COL),
            P(),
            P(),
            P(),
            P(),
            P(),
            P(),
            P(),
        ),
        out_specs=(P(ROW_COL, None, None), P(ROW_COL, None)),
        check_vma=False,
    )
```

```python
import functools

import jax
import jax.numpy as jnp
from jax import lax
from jax.experimental import pallas as pl
from jax.experimental.pallas import tpu as pltpu
from jax.sharding import Mesh
from jax.sharding import PartitionSpec as P

G_DEV = 32
READ_DEV = 8
ROW_COL = ("row", "col_0", "col_1", "col_2")
CHIP = ("row", "col_0", "col_1")
SWAP = [(0, 1), (1, 0)]
PACK_BITS = 3
PACK = 1 << PACK_BITS
POOL = 8
MLP_BITS = 3
HEAD_ROWS = 80
TAIL_BITS = 4
TAIL_GRAPHS = 1 << TAIL_BITS
MLP = 1 << MLP_BITS
VMEM_BYTES = 59 * 1024 * 1024
FINISH_BYTES = 40 * 1024 * 1024
BLEND_BYTES = 56 * 1024 * 1024


def masked_sum(keep, values, axis):
    return jnp.sum(jnp.where(keep, values, 0), axis=axis)


def info_kernel(live, counts, ids, out):
    rows, size = out.shape[0], counts.shape[1]
    for lane, values in ((0, counts), (size, ids)):
        out[:, :, lane : lane + size] = jnp.broadcast_to(values[...][None], (rows, 1, size))
    out[:, :, 2 * size :] = jnp.full((rows, 1, 1), live[0], jnp.int32)


def info_rows(live, counts, ids, devices):
    vector = pl.BlockSpec(memory_space=pltpu.VMEM)
    return pl.pallas_call(
        info_kernel,
        out_shape=jax.ShapeDtypeStruct((devices, 1, 2 * counts.shape[1] + 1), jnp.int32),
        in_specs=[pl.BlockSpec(memory_space=pltpu.SMEM), vector, vector],
        out_specs=vector,
        name="info",
    )(live, counts, ids)


def blend_kernel(
    first,
    where,
    scale,
    live,
    own,
    par,
    own_edges_from,
    par_edges_from,
    out,
    taken,
    made,
    own_edges,
    par_edges,
    taken_sem,
    made_sem,
    edge_sem,
):
    edge_copies = [
        pltpu.make_async_copy(own_edges_from, own_edges, edge_sem.at[0]),
        pltpu.make_async_copy(par_edges_from, par_edges, edge_sem.at[1]),
    ]
    for copy in edge_copies:
        copy.start()
    chip, core = where[0], where[1]
    device = lax.broadcasted_iota(jnp.int32, live.shape, 1)

    def total(keep):
        return jnp.sum(jnp.where(keep, live[...].astype(jnp.float32), 0.0)).astype(jnp.int32)

    offset = total(device < 2 * chip)
    live_a = total(device == 2 * chip)
    live_b = total(device == 2 * chip + 1)
    count, nodes, _ = taken.shape
    size = made.shape[1]
    wrap = 2 * count - 1
    node_index = lax.broadcasted_iota(jnp.int32, (nodes, own_edges.shape[-1]), 0)
    row_index = first + lax.broadcasted_iota(jnp.int32, (size, own_edges.shape[-1]), 0)

    def source_of(slot):
        number = (2 * slot + core - offset) & wrap
        filled = number < live_a + live_b
        from_b = number >= live_a
        index = jnp.where(filled, jnp.where(from_b, number - live_a, number), slot)
        return index, jnp.logical_xor(from_b, core == 1)

    @pl.loop(0, count)
    def _(slot):
        index, from_par = source_of(slot)
        sem = taken_sem.at[slot >> PACK_BITS]

        @pl.when(from_par)
        def _():
            pltpu.make_async_copy(par.at[index], taken.at[slot], sem).start()

        @pl.when(jnp.logical_not(from_par))
        def _():
            pltpu.make_async_copy(own.at[index], taken.at[slot], sem).start()

    def put(group):
        rows = pl.ds(group * PACK, PACK)
        return pltpu.make_async_copy(made.at[rows], out.at[rows], made_sem.at[group])

    for copy in edge_copies:
        copy.wait()

    @pl.loop(0, count // PACK)
    def _(group):
        pltpu.make_async_copy(
            own.at[pl.ds(0, PACK)], taken.at[pl.ds(group * PACK, PACK)], taken_sem.at[group]
        ).wait()
        slots = [group * PACK + lane for lane in range(PACK)]
        sources, targets = [], []
        for slot in slots:
            index, from_par = source_of(slot)
            edges = jnp.where(from_par, par_edges[index], own_edges[index])
            sources.append((node_index == edges[0:1, :]).astype(jnp.bfloat16))
            targets.append((row_index == edges[1:2, :]).astype(jnp.bfloat16))
        adjacency = [
            lax.dot_general(t, s, (((1,), (1,)), ((), ())), preferred_element_type=jnp.float32)
            for t, s in zip(targets, sources)
        ]
        features = [taken[slot] for slot in slots]
        neighbours = [
            jnp.dot(a.astype(jnp.bfloat16), f, preferred_element_type=jnp.float32)
            for a, f in zip(adjacency, features)
        ]
        for slot, f, n in zip(slots, features, neighbours):
            kept = f[first : first + size].astype(jnp.float32)
            made[slot] = (scale[0] * kept + n).astype(jnp.bfloat16)
        put(group).start()

    @pl.loop(0, count // PACK)
    def _(group):
        put(group).wait()


def blended_slots(own, par, own_edges, par_edges, where, live, scale, first, size):
    count, nodes, hidden = own.shape
    anywhere = pl.BlockSpec(memory_space=pl.ANY)
    vector = pl.BlockSpec(memory_space=pltpu.VMEM)
    scalar = pl.BlockSpec(memory_space=pltpu.SMEM)
    return pl.pallas_call(
        functools.partial(blend_kernel, first),
        out_shape=jax.ShapeDtypeStruct((count, size, hidden), jnp.bfloat16),
        in_specs=[scalar, scalar, vector] + [anywhere] * 4,
        out_specs=anywhere,
        scratch_shapes=[
            pltpu.VMEM((count, nodes, hidden), jnp.bfloat16),
            pltpu.VMEM((count, size, hidden), jnp.bfloat16),
            pltpu.VMEM(own_edges.shape, jnp.int32),
            pltpu.VMEM(own_edges.shape, jnp.int32),
            pltpu.SemaphoreType.DMA((count // PACK,)),
            pltpu.SemaphoreType.DMA((count // PACK,)),
            pltpu.SemaphoreType.DMA((2,)),
        ],
        compiler_params=pltpu.CompilerParams(vmem_limit_bytes=BLEND_BYTES),
        cost_estimate=pl.CostEstimate(
            flops=2 * count * size * nodes * (own_edges.shape[-1] + hidden),
            bytes_accessed=4 * count * nodes * hidden,
            transcendentals=0,
        ),
        name="blend",
    )(where, scale, live, own, par, own_edges, par_edges)


def perceptron(rows, weights):
    w_first, b_first, w_second, b_second, w_third, b_third = weights
    for w, b in ((w_first, b_first), (w_second, b_second)):
        total = jnp.dot(rows, w[...], preferred_element_type=jnp.float32) + b[...]
        rows = jnp.maximum(total, 0.0).astype(jnp.bfloat16)
    return jnp.dot(rows, w_third[...], preferred_element_type=jnp.float32) + b_third[...]


def weight_specs(weights):
    return [pl.BlockSpec(w.shape, lambda i, *tables: (0, 0)) for w in weights]


def mlp_cost(rows, hidden):
    return pl.CostEstimate(
        flops=6 * rows * hidden * hidden, bytes_accessed=4 * rows * hidden, transcendentals=0
    )


def pool_kernel(counts, head_ref, tail_ref, *refs):
    weights, out = refs[:6], refs[6]
    step = pl.program_id(0)
    many, head, hidden = head_ref.shape
    tail = tail_ref.shape[1]
    rows = jnp.concatenate(
        [head_ref[...].reshape(many * head, hidden), tail_ref[...].reshape(many * tail, hidden)],
        axis=0,
    )
    result = perceptron(rows, weights)
    for lane in range(many):
        count = counts[step * many + lane]
        total = jnp.zeros((1, hidden), jnp.float32)
        for first, start, size in ((0, lane * head, head), (head, many * head + lane * tail, tail)):
            node_index = first + lax.broadcasted_iota(jnp.int32, (size, 1), 0)
            kept = jnp.where(node_index < count, result[start : start + size], 0.0)
            kept = kept.astype(jnp.bfloat16).astype(jnp.float32)
            total = total + jnp.sum(kept, axis=0, keepdims=True)
        out[lane : lane + 1, :] = total / jnp.maximum(count, 1).astype(jnp.float32)


def pooled_slots(heads, tails, counts, weights):
    count, head, hidden = heads.shape
    tail = tails.shape[1]
    return pl.pallas_call(
        pool_kernel,
        out_shape=jax.ShapeDtypeStruct((count, hidden), jnp.float32),
        grid_spec=pltpu.PrefetchScalarGridSpec(
            num_scalar_prefetch=1,
            grid=(count // POOL,),
            in_specs=[
                pl.BlockSpec((POOL, head, hidden), lambda i, *tables: (i, 0, 0)),
                pl.BlockSpec((POOL, tail, hidden), lambda i, *tables: (i, 0, 0)),
            ]
            + weight_specs(weights),
            out_specs=pl.BlockSpec((POOL, hidden), lambda i, *tables: (i, 0)),
        ),
        compiler_params=pltpu.CompilerParams(dimension_semantics=("arbitrary",)),
        cost_estimate=mlp_cost(count * (head + tail), hidden),
        name="pool",
    )(counts, heads, tails, *weights)


def place_kernel(chips, counts, arrived, *refs):
    weights, out, taken, made, taken_sem, made_sem = refs[:6], *refs[6:]
    count, nodes, hidden = taken.shape

    @pl.loop(0, count)
    def _(slot):
        pltpu.make_async_copy(
            arrived.at[chips[slot]], taken.at[slot], taken_sem.at[slot >> MLP_BITS]
        ).start()

    def put(group):
        rows = pl.ds(group * MLP, MLP)
        return pltpu.make_async_copy(
            made.at[rows], out.at[rows, pl.ds(0, nodes)], made_sem.at[group]
        )

    node_index = lax.broadcasted_iota(jnp.int32, (nodes, 1), 0)

    @pl.loop(0, count // MLP)
    def _(group):
        rows = pl.ds(group * MLP, MLP)
        pltpu.make_async_copy(
            arrived.at[pl.ds(0, MLP)], taken.at[rows], taken_sem.at[group]
        ).wait()
        result = perceptron(taken[rows].reshape(MLP * nodes, hidden), weights)
        for lane in range(MLP):
            slot = group * MLP + lane
            part = result[lane * nodes : (lane + 1) * nodes]
            made[slot] = jnp.where(node_index < counts[slot], part, 0.0).astype(jnp.bfloat16)
        put(group).start()

    @pl.loop(0, count // MLP)
    def _(group):
        put(group).wait()


def placed_heads(arrived, chips, counts, weights, nodes):
    _, head, hidden = arrived.shape
    anywhere = pl.BlockSpec(memory_space=pl.ANY)
    vector = pl.BlockSpec(memory_space=pltpu.VMEM)
    scalar = pl.BlockSpec(memory_space=pltpu.SMEM)
    return pl.pallas_call(
        place_kernel,
        out_shape=jax.ShapeDtypeStruct((G_DEV, nodes, hidden), jnp.bfloat16),
        in_specs=[scalar, scalar, anywhere] + [vector] * 6,
        out_specs=anywhere,
        scratch_shapes=[
            pltpu.VMEM((G_DEV, head, hidden), jnp.bfloat16),
            pltpu.VMEM((G_DEV, head, hidden), jnp.bfloat16),
            pltpu.SemaphoreType.DMA((G_DEV // MLP,)),
            pltpu.SemaphoreType.DMA((G_DEV // MLP,)),
        ],
        compiler_params=pltpu.CompilerParams(vmem_limit_bytes=VMEM_BYTES),
        cost_estimate=mlp_cost(G_DEV * head, hidden),
        name="place",
    )(chips, counts, arrived, *weights)


def finish_kernel(chips, counts, arrived, *refs):
    weights, refs = refs[:6], refs[7:]
    out, readout, taken, made, terms, taken_sem, made_sem, terms_sem = refs
    count, tail, hidden = taken.shape
    nodes = out.shape[1]
    own_rows = pl.ds(0, tail)

    @pl.loop(0, count)
    def _(slot):
        pltpu.make_async_copy(
            arrived.at[chips[slot], own_rows], taken.at[slot], taken_sem.at[slot >> TAIL_BITS]
        ).start()

    summed = pltpu.make_async_copy(arrived.at[:, pl.ds(tail, READ_DEV)], terms, terms_sem)
    summed.start()

    def put(group):
        rows = pl.ds(group * TAIL_GRAPHS, TAIL_GRAPHS)
        return pltpu.make_async_copy(
            made.at[rows], out.at[rows, pl.ds(nodes - tail, tail)], made_sem.at[group]
        )

    node_index = nodes - tail + lax.broadcasted_iota(jnp.int32, (tail, 1), 0)

    @pl.loop(0, count // TAIL_GRAPHS)
    def _(group):
        rows = pl.ds(group * TAIL_GRAPHS, TAIL_GRAPHS)
        pltpu.make_async_copy(
            arrived.at[pl.ds(0, TAIL_GRAPHS), own_rows], taken.at[rows], taken_sem.at[group]
        ).wait()
        result = perceptron(taken[rows].reshape(TAIL_GRAPHS * tail, hidden), weights)
        for lane in range(TAIL_GRAPHS):
            slot = group * TAIL_GRAPHS + lane
            part = result[lane * tail : (lane + 1) * tail]
            made[slot] = jnp.where(node_index < counts[slot], part, 0.0).astype(jnp.bfloat16)
        put(group).start()

    summed.wait()
    readout[...] = jnp.sum(terms[...].astype(jnp.float32), axis=0)

    @pl.loop(0, count // TAIL_GRAPHS)
    def _(group):
        put(group).wait()


def finished(node_out, arrived, chips, counts, weights):
    count, nodes, hidden = node_out.shape
    tail = arrived.shape[1] - READ_DEV
    anywhere = pl.BlockSpec(memory_space=pl.ANY)
    vector = pl.BlockSpec(memory_space=pltpu.VMEM)
    scalar = pl.BlockSpec(memory_space=pltpu.SMEM)
    return pl.pallas_call(
        finish_kernel,
        out_shape=[
            jax.ShapeDtypeStruct(node_out.shape, jnp.bfloat16),
            jax.ShapeDtypeStruct((READ_DEV, hidden), jnp.float32),
        ],
        in_specs=[scalar, scalar, anywhere] + [vector] * 6 + [anywhere],
        out_specs=[anywhere, vector],
        scratch_shapes=[
            pltpu.VMEM((count, tail, hidden), jnp.bfloat16),
            pltpu.VMEM((count, tail, hidden), jnp.bfloat16),
            pltpu.VMEM((arrived.shape[0], READ_DEV, hidden), jnp.bfloat16),
            pltpu.SemaphoreType.DMA((count // TAIL_GRAPHS,)),
            pltpu.SemaphoreType.DMA((count // TAIL_GRAPHS,)),
            pltpu.SemaphoreType.DMA,
        ],
        input_output_aliases={9: 0},
        compiler_params=pltpu.CompilerParams(vmem_limit_bytes=FINISH_BYTES),
        cost_estimate=mlp_cost(count * tail, hidden),
        name="finish",
    )(chips, counts, arrived, *weights, node_out)


def body(
    node_features,
    node_counts,
    edge_list,
    readout_ids,
    live_graphs,
    self_weight,
    w_first,
    b_first,
    w_second,
    b_second,
    w_third,
    b_third,
):
    weights = (
        w_first,
        b_first[None, :],
        w_second,
        b_second[None, :],
        w_third,
        b_third[None, :],
    )
    devices = lax.axis_size(ROW_COL)
    capacity, nodes, hidden = node_features.shape
    me = lax.axis_index(ROW_COL)
    core = lax.axis_index("col_2")
    chip = lax.axis_index(CHIP)

    par_features = lax.ppermute(node_features, "col_2", SWAP)
    par_edges = lax.ppermute(edge_list, "col_2", SWAP)
    info = info_rows(live_graphs, node_counts[None, :], readout_ids[None, :], devices)
    table = lax.all_to_all(info, ROW_COL, 0, 0, tiled=True)[:, 0]
    live = table[:, 2 * capacity]

    where = jnp.stack([chip, core])
    graphs = (node_features, par_features, edge_list, par_edges, where, live[None, :], self_weight)
    heads = blended_slots(*graphs, 0, HEAD_ROWS)
    arrived = lax.all_to_all(heads, CHIP, split_axis=0, concat_axis=0, tiled=True)
    tails = blended_slots(*graphs, HEAD_ROWS, nodes - HEAD_ROWS)

    device = lax.broadcasted_iota(jnp.int32, (3, devices), 1)
    part = lax.broadcasted_iota(jnp.int32, (3, devices), 0)
    ahead = (part == 0) & (device < 2 * chip)
    mine = (part >= 1) & (device == 2 * chip + part - 1)
    sums = masked_sum(ahead | mine, live[None, :], 1)
    offset, live_a, live_b = sums[0], sums[1], sums[2]
    slot = lax.broadcasted_iota(jnp.int32, (devices // 2,), 0)
    number = (2 * slot + core - offset) & (devices - 1)
    filled = number < live_a + live_b
    picked = jnp.where(number >= live_a, capacity + number - live_a, number)
    pair = lax.dynamic_slice_in_dim(table, 2 * chip, 2, 0)
    spot = lax.broadcasted_iota(jnp.int32, (devices // 2, 2 * capacity), 1) == picked[:, None]
    spot = spot & filled[:, None]
    slot_counts = masked_sum(spot, pair[:, :capacity].reshape(1, -1), 1)
    slot_ids = masked_sum(spot, pair[:, capacity : 2 * capacity].reshape(1, -1), 1)
    slot_ids = jnp.where(filled, slot_ids, -1)
    pooled = pooled_slots(heads, tails, slot_counts, weights)
    groups = READ_DEV * devices
    id_keys = lax.broadcasted_iota(jnp.int32, (groups, slot_ids.shape[0]), 0)
    members = (id_keys == slot_ids[None, :]).astype(jnp.float32)
    terms = jnp.dot(
        members, pooled, precision=lax.Precision.HIGHEST, preferred_element_type=jnp.float32
    )
    terms = terms.reshape(devices // 2, 2, READ_DEV, hidden)
    kept = lax.dynamic_index_in_dim(terms, core, 1, keepdims=False)
    sent = lax.dynamic_index_in_dim(terms, 1 - core, 1, keepdims=False).astype(jnp.bfloat16)
    both = kept + lax.ppermute(sent, "col_2", SWAP).astype(jnp.float32)
    rest = jnp.concatenate([tails, both.astype(jnp.bfloat16)], axis=1)
    rest, arrived = lax.optimization_barrier((rest, arrived))
    arrived_rest = lax.all_to_all(rest, CHIP, split_axis=0, concat_axis=0, tiled=True)

    order = lax.broadcasted_iota(jnp.int32, (G_DEV, 1), 0) * devices + me
    shape = (devices, devices)
    before = lax.broadcasted_iota(jnp.int32, shape, 1) <= lax.broadcasted_iota(jnp.int32, shape, 0)
    upto = masked_sum(before, live[None, :], 1)
    passed = upto[None, :] <= order
    source = jnp.sum(passed.astype(jnp.int32), axis=1)
    start = jnp.max(jnp.where(passed, upto[None, :], 0), axis=1)
    source_idx = order[:, 0] - start
    every = lax.broadcasted_iota(jnp.int32, (devices,), 0)
    hit = (every[None, :, None] == source[:, None, None]) & (
        lax.broadcasted_iota(jnp.int32, (1, 1, capacity), 2) == source_idx[:, None, None]
    )
    counts = jnp.sum(jnp.where(hit, table[None, :, :capacity], 0), axis=(1, 2))
    chips = source >> 1
    node_out = placed_heads(arrived, chips, counts, weights, nodes)
    return tuple(finished(node_out, arrived_rest, chips, counts, weights))


def solution(mesh):
    split = Mesh(
        mesh.devices.reshape(mesh.shape["row"], 4, 4, 2), ("row", "col_0", "col_1", "col_2")
    )
    return jax.shard_map(
        body,
        mesh=split,
        in_specs=(
            P(ROW_COL, None, None),
            P(ROW_COL),
            P(ROW_COL, None, None),
            P(ROW_COL),
            P(ROW_COL),
            P(),
            P(),
            P(),
            P(),
            P(),
            P(),
            P(),
        ),
        out_specs=(P(ROW_COL, None, None), P(ROW_COL, None)),
        check_vma=False,
    )
```

```python
import functools

import jax
import jax.numpy as jnp
from jax import lax
from jax.experimental import pallas as pl
from jax.experimental.pallas import tpu as pltpu
from jax.sharding import Mesh
from jax.sharding import PartitionSpec as P

G_DEV = 32
READ_DEV = 8
ROW_COL = ("row", "col_0", "col_1", "col_2")
CHIP = ("row", "col_0", "col_1")
SWAP = [(0, 1), (1, 0)]
PACK_BITS = 3
PACK = 1 << PACK_BITS
POOL = 8
MLP_BITS = 3
HEAD_ROWS = 72
TAIL_BITS = 4
TAIL_GRAPHS = 1 << TAIL_BITS
MLP = 1 << MLP_BITS
VMEM_BYTES = 59 * 1024 * 1024
FINISH_BYTES = 40 * 1024 * 1024
BLEND_BYTES = 56 * 1024 * 1024


def masked_sum(keep, values, axis):
    return jnp.sum(jnp.where(keep, values, 0), axis=axis)


def blend_kernel(
    first, where, scale, own, par, own_edges, par_edges, out, taken, made, taken_sem, made_sem
):
    core, offset, live_a, live_b = where[0], where[1], where[2], where[3]
    count, nodes, _ = taken.shape
    size = made.shape[1]
    wrap = 2 * count - 1
    node_index = lax.broadcasted_iota(jnp.int32, (nodes, own_edges.shape[-1]), 0)
    row_index = first + lax.broadcasted_iota(jnp.int32, (size, own_edges.shape[-1]), 0)

    def source_of(slot):
        number = (2 * slot + core - offset) & wrap
        filled = number < live_a + live_b
        from_b = number >= live_a
        index = jnp.where(filled, jnp.where(from_b, number - live_a, number), slot)
        return index, jnp.logical_xor(from_b, core == 1)

    @pl.loop(0, count)
    def _(slot):
        index, from_par = source_of(slot)
        sem = taken_sem.at[slot >> PACK_BITS]

        @pl.when(from_par)
        def _():
            pltpu.make_async_copy(par.at[index], taken.at[slot], sem).start()

        @pl.when(jnp.logical_not(from_par))
        def _():
            pltpu.make_async_copy(own.at[index], taken.at[slot], sem).start()

    def put(group):
        rows = pl.ds(group * PACK, PACK)
        return pltpu.make_async_copy(made.at[rows], out.at[rows], made_sem.at[group])

    @pl.loop(0, count // PACK)
    def _(group):
        pltpu.make_async_copy(
            own.at[pl.ds(0, PACK)], taken.at[pl.ds(group * PACK, PACK)], taken_sem.at[group]
        ).wait()
        slots = [group * PACK + lane for lane in range(PACK)]
        sources, targets = [], []
        for slot in slots:
            index, from_par = source_of(slot)
            edges = jnp.where(from_par, par_edges[index], own_edges[index])
            sources.append((node_index == edges[0:1, :]).astype(jnp.bfloat16))
            targets.append((row_index == edges[1:2, :]).astype(jnp.bfloat16))
        adjacency = [
            lax.dot_general(t, s, (((1,), (1,)), ((), ())), preferred_element_type=jnp.float32)
            for t, s in zip(targets, sources)
        ]
        features = [taken[slot] for slot in slots]
        neighbours = [
            jnp.dot(a.astype(jnp.bfloat16), f, preferred_element_type=jnp.float32)
            for a, f in zip(adjacency, features)
        ]
        for slot, f, n in zip(slots, features, neighbours):
            kept = f[first : first + size].astype(jnp.float32)
            made[slot] = (scale[0] * kept + n).astype(jnp.bfloat16)
        put(group).start()

    @pl.loop(0, count // PACK)
    def _(group):
        put(group).wait()


def blended_slots(own, par, own_edges, par_edges, where, scale, first, size):
    count, nodes, hidden = own.shape
    anywhere = pl.BlockSpec(memory_space=pl.ANY)
    vector = pl.BlockSpec(memory_space=pltpu.VMEM)
    scalar = pl.BlockSpec(memory_space=pltpu.SMEM)
    return pl.pallas_call(
        functools.partial(blend_kernel, first),
        out_shape=jax.ShapeDtypeStruct((count, size, hidden), jnp.bfloat16),
        in_specs=[scalar, scalar, anywhere, anywhere, vector, vector],
        out_specs=anywhere,
        scratch_shapes=[
            pltpu.VMEM((count, nodes, hidden), jnp.bfloat16),
            pltpu.VMEM((count, size, hidden), jnp.bfloat16),
            pltpu.SemaphoreType.DMA((count // PACK,)),
            pltpu.SemaphoreType.DMA((count // PACK,)),
        ],
        compiler_params=pltpu.CompilerParams(vmem_limit_bytes=BLEND_BYTES),
        cost_estimate=pl.CostEstimate(
            flops=2 * count * size * nodes * (own_edges.shape[-1] + hidden),
            bytes_accessed=4 * count * nodes * hidden,
            transcendentals=0,
        ),
        name="blend",
    )(where, scale, own, par, own_edges, par_edges)


def perceptron(rows, weights):
    w_first, b_first, w_second, b_second, w_third, b_third = weights
    for w, b in ((w_first, b_first), (w_second, b_second)):
        total = jnp.dot(rows, w[...], preferred_element_type=jnp.float32) + b[...]
        rows = jnp.maximum(total, 0.0).astype(jnp.bfloat16)
    return jnp.dot(rows, w_third[...], preferred_element_type=jnp.float32) + b_third[...]


def weight_specs(weights):
    return [pl.BlockSpec(w.shape, lambda i, *tables: (0, 0)) for w in weights]


def mlp_cost(rows, hidden):
    return pl.CostEstimate(
        flops=6 * rows * hidden * hidden, bytes_accessed=4 * rows * hidden, transcendentals=0
    )


def pool_kernel(counts, head_ref, tail_ref, *refs):
    weights, out = refs[:6], refs[6]
    step = pl.program_id(0)
    many, head, hidden = head_ref.shape
    tail = tail_ref.shape[1]
    rows = jnp.concatenate(
        [head_ref[...].reshape(many * head, hidden), tail_ref[...].reshape(many * tail, hidden)],
        axis=0,
    )
    result = perceptron(rows, weights)
    for lane in range(many):
        count = counts[step * many + lane]
        total = jnp.zeros((1, hidden), jnp.float32)
        for first, start, size in ((0, lane * head, head), (head, many * head + lane * tail, tail)):
            node_index = first + lax.broadcasted_iota(jnp.int32, (size, 1), 0)
            kept = jnp.where(node_index < count, result[start : start + size], 0.0)
            kept = kept.astype(jnp.bfloat16).astype(jnp.float32)
            total = total + jnp.sum(kept, axis=0, keepdims=True)
        out[lane : lane + 1, :] = total / jnp.maximum(count, 1).astype(jnp.float32)


def pooled_slots(heads, tails, counts, weights):
    count, head, hidden = heads.shape
    tail = tails.shape[1]
    return pl.pallas_call(
        pool_kernel,
        out_shape=jax.ShapeDtypeStruct((count, hidden), jnp.float32),
        grid_spec=pltpu.PrefetchScalarGridSpec(
            num_scalar_prefetch=1,
            grid=(count // POOL,),
            in_specs=[
                pl.BlockSpec((POOL, head, hidden), lambda i, *tables: (i, 0, 0)),
                pl.BlockSpec((POOL, tail, hidden), lambda i, *tables: (i, 0, 0)),
            ]
            + weight_specs(weights),
            out_specs=pl.BlockSpec((POOL, hidden), lambda i, *tables: (i, 0)),
        ),
        compiler_params=pltpu.CompilerParams(dimension_semantics=("arbitrary",)),
        cost_estimate=mlp_cost(count * (head + tail), hidden),
        name="pool",
    )(counts, heads, tails, *weights)


def place_kernel(chips, counts, arrived, *refs):
    weights, out, taken, made, taken_sem, made_sem = refs[:6], *refs[6:]
    count, nodes, hidden = taken.shape

    @pl.loop(0, count)
    def _(slot):
        pltpu.make_async_copy(
            arrived.at[chips[slot]], taken.at[slot], taken_sem.at[slot >> MLP_BITS]
        ).start()

    def put(group):
        rows = pl.ds(group * MLP, MLP)
        return pltpu.make_async_copy(
            made.at[rows], out.at[rows, pl.ds(0, nodes)], made_sem.at[group]
        )

    node_index = lax.broadcasted_iota(jnp.int32, (nodes, 1), 0)

    @pl.loop(0, count // MLP)
    def _(group):
        rows = pl.ds(group * MLP, MLP)
        pltpu.make_async_copy(
            arrived.at[pl.ds(0, MLP)], taken.at[rows], taken_sem.at[group]
        ).wait()
        result = perceptron(taken[rows].reshape(MLP * nodes, hidden), weights)
        for lane in range(MLP):
            slot = group * MLP + lane
            part = result[lane * nodes : (lane + 1) * nodes]
            made[slot] = jnp.where(node_index < counts[slot], part, 0.0).astype(jnp.bfloat16)
        put(group).start()

    @pl.loop(0, count // MLP)
    def _(group):
        put(group).wait()


def placed_heads(arrived, chips, counts, weights, nodes):
    _, head, hidden = arrived.shape
    anywhere = pl.BlockSpec(memory_space=pl.ANY)
    vector = pl.BlockSpec(memory_space=pltpu.VMEM)
    scalar = pl.BlockSpec(memory_space=pltpu.SMEM)
    return pl.pallas_call(
        place_kernel,
        out_shape=jax.ShapeDtypeStruct((G_DEV, nodes, hidden), jnp.bfloat16),
        in_specs=[scalar, scalar, anywhere] + [vector] * 6,
        out_specs=anywhere,
        scratch_shapes=[
            pltpu.VMEM((G_DEV, head, hidden), jnp.bfloat16),
            pltpu.VMEM((G_DEV, head, hidden), jnp.bfloat16),
            pltpu.SemaphoreType.DMA((G_DEV // MLP,)),
            pltpu.SemaphoreType.DMA((G_DEV // MLP,)),
        ],
        compiler_params=pltpu.CompilerParams(vmem_limit_bytes=VMEM_BYTES),
        cost_estimate=mlp_cost(G_DEV * head, hidden),
        name="place",
    )(chips, counts, arrived, *weights)


def finish_kernel(chips, counts, arrived, *refs):
    weights, refs = refs[:6], refs[7:]
    out, readout, taken, made, terms, taken_sem, made_sem, terms_sem = refs
    count, tail, hidden = taken.shape
    nodes = out.shape[1]
    own_rows = pl.ds(0, tail)

    @pl.loop(0, count)
    def _(slot):
        pltpu.make_async_copy(
            arrived.at[chips[slot], own_rows], taken.at[slot], taken_sem.at[slot >> TAIL_BITS]
        ).start()

    summed = pltpu.make_async_copy(arrived.at[:, pl.ds(tail, READ_DEV)], terms, terms_sem)
    summed.start()

    def put(group):
        rows = pl.ds(group * TAIL_GRAPHS, TAIL_GRAPHS)
        return pltpu.make_async_copy(
            made.at[rows], out.at[rows, pl.ds(nodes - tail, tail)], made_sem.at[group]
        )

    node_index = nodes - tail + lax.broadcasted_iota(jnp.int32, (tail, 1), 0)

    @pl.loop(0, count // TAIL_GRAPHS)
    def _(group):
        rows = pl.ds(group * TAIL_GRAPHS, TAIL_GRAPHS)
        pltpu.make_async_copy(
            arrived.at[pl.ds(0, TAIL_GRAPHS), own_rows], taken.at[rows], taken_sem.at[group]
        ).wait()
        result = perceptron(taken[rows].reshape(TAIL_GRAPHS * tail, hidden), weights)
        for lane in range(TAIL_GRAPHS):
            slot = group * TAIL_GRAPHS + lane
            part = result[lane * tail : (lane + 1) * tail]
            made[slot] = jnp.where(node_index < counts[slot], part, 0.0).astype(jnp.bfloat16)
        put(group).start()

    summed.wait()
    readout[...] = jnp.sum(terms[...].astype(jnp.float32), axis=0)

    @pl.loop(0, count // TAIL_GRAPHS)
    def _(group):
        put(group).wait()


def finished(node_out, arrived, chips, counts, weights):
    count, nodes, hidden = node_out.shape
    tail = arrived.shape[1] - READ_DEV
    anywhere = pl.BlockSpec(memory_space=pl.ANY)
    vector = pl.BlockSpec(memory_space=pltpu.VMEM)
    scalar = pl.BlockSpec(memory_space=pltpu.SMEM)
    return pl.pallas_call(
        finish_kernel,
        out_shape=[
            jax.ShapeDtypeStruct(node_out.shape, jnp.bfloat16),
            jax.ShapeDtypeStruct((READ_DEV, hidden), jnp.float32),
        ],
        in_specs=[scalar, scalar, anywhere] + [vector] * 6 + [anywhere],
        out_specs=[anywhere, vector],
        scratch_shapes=[
            pltpu.VMEM((count, tail, hidden), jnp.bfloat16),
            pltpu.VMEM((count, tail, hidden), jnp.bfloat16),
            pltpu.VMEM((arrived.shape[0], READ_DEV, hidden), jnp.bfloat16),
            pltpu.SemaphoreType.DMA((count // TAIL_GRAPHS,)),
            pltpu.SemaphoreType.DMA((count // TAIL_GRAPHS,)),
            pltpu.SemaphoreType.DMA,
        ],
        input_output_aliases={9: 0},
        compiler_params=pltpu.CompilerParams(vmem_limit_bytes=FINISH_BYTES),
        cost_estimate=mlp_cost(count * tail, hidden),
        name="finish",
    )(chips, counts, arrived, *weights, node_out)


def body(
    node_features,
    node_counts,
    edge_list,
    readout_ids,
    live_graphs,
    self_weight,
    w_first,
    b_first,
    w_second,
    b_second,
    w_third,
    b_third,
):
    weights = (
        w_first,
        b_first[None, :],
        w_second,
        b_second[None, :],
        w_third,
        b_third[None, :],
    )
    devices = lax.axis_size(ROW_COL)
    capacity, nodes, hidden = node_features.shape
    me = lax.axis_index(ROW_COL)
    core = lax.axis_index("col_2")
    chip = lax.axis_index(CHIP)

    par_features = lax.ppermute(node_features, "col_2", SWAP)
    par_edges = lax.ppermute(edge_list, "col_2", SWAP)
    info = jnp.concatenate([live_graphs, node_counts, readout_ids])
    table = lax.all_to_all(
        jnp.broadcast_to(info[None], (devices, info.shape[0])), ROW_COL, 0, 0, tiled=True
    )
    live = table[:, 0]

    device = lax.broadcasted_iota(jnp.int32, (4, devices), 1)
    part = lax.broadcasted_iota(jnp.int32, (4, devices), 0)
    ahead = (part == 1) & (device < 2 * chip)
    mine = (part >= 2) & (device == 2 * chip + part - 2)
    own = (part == 0) & (device < core)
    place = masked_sum(ahead | mine | own, jnp.where(own, 1, live[None, :]), 1)

    graphs = (node_features, par_features, edge_list, par_edges, place, self_weight)
    heads = blended_slots(*graphs, 0, HEAD_ROWS)
    arrived = lax.all_to_all(heads, CHIP, split_axis=0, concat_axis=0, tiled=True)
    tails = blended_slots(*graphs, HEAD_ROWS, nodes - HEAD_ROWS)

    offset, live_a, live_b = place[1], place[2], place[3]
    slot = lax.broadcasted_iota(jnp.int32, (devices // 2,), 0)
    number = (2 * slot + core - offset) & (devices - 1)
    filled = number < live_a + live_b
    picked = jnp.where(number >= live_a, capacity + number - live_a, number)
    pair = lax.dynamic_slice_in_dim(table, 2 * chip, 2, 0)
    spot = lax.broadcasted_iota(jnp.int32, (devices // 2, 2 * capacity), 1) == picked[:, None]
    spot = spot & filled[:, None]
    slot_counts = masked_sum(spot, pair[:, 1 : 1 + capacity].reshape(1, -1), 1)
    slot_ids = masked_sum(spot, pair[:, 1 + capacity :].reshape(1, -1), 1)
    slot_ids = jnp.where(filled, slot_ids, -1)
    pooled = pooled_slots(heads, tails, slot_counts, weights)
    groups = READ_DEV * devices
    id_keys = lax.broadcasted_iota(jnp.int32, (groups, slot_ids.shape[0]), 0)
    members = (id_keys == slot_ids[None, :]).astype(jnp.float32)
    terms = jnp.dot(
        members, pooled, precision=lax.Precision.HIGHEST, preferred_element_type=jnp.float32
    )
    terms = terms.reshape(devices // 2, 2, READ_DEV, hidden)
    kept = lax.dynamic_index_in_dim(terms, core, 1, keepdims=False)
    sent = lax.dynamic_index_in_dim(terms, 1 - core, 1, keepdims=False).astype(jnp.bfloat16)
    both = kept + lax.ppermute(sent, "col_2", SWAP).astype(jnp.float32)
    rest = jnp.concatenate([tails, both.astype(jnp.bfloat16)], axis=1)
    rest, arrived = lax.optimization_barrier((rest, arrived))
    arrived_rest = lax.all_to_all(rest, CHIP, split_axis=0, concat_axis=0, tiled=True)

    order = lax.broadcasted_iota(jnp.int32, (G_DEV, 1), 0) * devices + me
    shape = (devices, devices)
    before = lax.broadcasted_iota(jnp.int32, shape, 1) <= lax.broadcasted_iota(jnp.int32, shape, 0)
    upto = masked_sum(before, live[None, :], 1)
    passed = upto[None, :] <= order
    source = jnp.sum(passed.astype(jnp.int32), axis=1)
    start = jnp.max(jnp.where(passed, upto[None, :], 0), axis=1)
    source_idx = order[:, 0] - start
    every = lax.broadcasted_iota(jnp.int32, (devices,), 0)
    hit = (every[None, :, None] == source[:, None, None]) & (
        lax.broadcasted_iota(jnp.int32, (1, 1, capacity), 2) == source_idx[:, None, None]
    )
    counts = jnp.sum(jnp.where(hit, table[None, :, 1 : 1 + capacity], 0), axis=(1, 2))
    chips = source >> 1
    node_out = placed_heads(arrived, chips, counts, weights, nodes)
    return tuple(finished(node_out, arrived_rest, chips, counts, weights))


def solution(mesh):
    split = Mesh(
        mesh.devices.reshape(mesh.shape["row"], 4, 4, 2), ("row", "col_0", "col_1", "col_2")
    )
    return jax.shard_map(
        body,
        mesh=split,
        in_specs=(
            P(ROW_COL, None, None),
            P(ROW_COL),
            P(ROW_COL, None, None),
            P(ROW_COL),
            P(ROW_COL),
            P(),
            P(),
            P(),
            P(),
            P(),
            P(),
            P(),
        ),
        out_specs=(P(ROW_COL, None, None), P(ROW_COL, None)),
        check_vma=False,
    )
```
